32 devices in a mesh: rep: 4 (over x, y), dp: 8 (over z, core).
Axes of the slice: x: 2, y: 2, z: 4, core: 2. Of those that a mesh axis runs over, the one named last changes fastest.
Arguments:
- x: bfloat16 [32, 2048, 640], P(('rep', 'dp')), parts along dimension 0
- dy: bfloat16 [32, 2048, 640], P(('rep', 'dp')), parts along dimension 0
- w_gate: bfloat16 [2, 640, 4096], replicated
- w_up: bfloat16 [2, 640, 4096], replicated
- w_down: bfloat16 [2, 4096, 640], replicated
- m_w_gate: float32 [2, 640, 4096], P(None, 'dp')
- m_w_up: float32 [2, 640, 4096], P(None, 'dp')
- m_w_down: float32 [2, 4096, 640], P(None, 'dp')
- v_w_gate: float32 [2, 640, 4096], P(None, 'dp')
- v_w_up: float32 [2, 640, 4096], P(None, 'dp')
- v_w_down: float32 [2, 4096, 640], P(None, 'dp')
Outputs:
- output 1: bfloat16 [8, 640, 4096], P('rep'), parts along dimension 0
- output 2: bfloat16 [8, 640, 4096], P('rep'), parts along dimension 0
- output 3: bfloat16 [8, 4096, 640], P('rep'), parts along dimension 0
- output 4: float32 [8, 640, 4096], P('rep', 'dp'), parts along dimension 0
- output 5: float32 [8, 640, 4096], P('rep', 'dp'), parts along dimension 0
- output 6: float32 [8, 4096, 640], P('rep', 'dp'), parts along dimension 0
- output 7: float32 [8, 640, 4096], P('rep', 'dp'), parts along dimension 0
- output 8: float32 [8, 640, 4096], P('rep', 'dp'), parts along dimension 0
- output 9: float32 [8, 4096, 640], P('rep', 'dp'), parts along dimension 0
There are 4 independent parts. The reference program is written for one: setup_inputs(seed, part) draws one part's arguments, and reference() takes and returns one part's arrays. A program takes and returns all parts, laid end to end along the dimension named above; an argument that names none is the same for every part.
All inputs are finite; a program needn't handle non-finite values.
Results may differ from the reference program's by a relative error of at most 0.022.
Values are sent between devices in bfloat16 or wider.
A program may use at most 2 GiB of HBM per device.

```python
import jax
import jax.numpy as jnp
from jax import lax

SEQUENCES = 8
TOKENS = 2048
D = 640
FF = 4096
LAYERS = 2
NAMES = ("w_gate", "w_up", "w_down")
SHAPES = {"w_gate": (LAYERS, D, FF), "w_up": (LAYERS, D, FF), "w_down": (LAYERS, FF, D)}


def bump(key, n, height):
    away = (jnp.arange(n, dtype=jnp.int32) - jax.random.randint(key, (), 0, n, jnp.int32)) % n
    return jnp.where(away < n // 8, height, 1.0)


def together(key, own, strength):
    shared = jax.random.normal(key, own.shape[1:], jnp.float32)
    return (own + strength * shared) * lax.rsqrt(1 + strength * strength)


def setup_inputs(seed: int = 0, part: int = 0) -> dict:
    kx, kdy, ka, kb, kz, kf, kh, kl, *keys = jax.random.split(jax.random.key(seed), 8 + 3 * len(NAMES))
    kx, kdy, ka, kb = (jax.random.fold_in(k, part) for k in (kx, kdy, ka, kb))
    kw, km, kv = (keys[i::3] for i in range(3))
    shape = (SEQUENCES, TOKENS, D)
    much_x, much_dy = jax.random.uniform(kz, (2,), jnp.float32, 0.0, 1.0)
    loud = 2.0 ** jax.random.uniform(jax.random.fold_in(kz, 1), (), jnp.float32, -1.0, 2.0)
    layers = 2.0 ** jax.random.uniform(kl, (LAYERS, 1, 1), jnp.float32, -1.0, 1.0)
    x = together(ka, jax.random.normal(kx, shape, jnp.float32), much_x) * bump(kf, D, 4.0)
    dy = together(kb, jax.random.normal(kdy, shape, jnp.float32), much_dy)
    drawn = {"x": x.astype(jnp.bfloat16), "dy": (loud * dy * (SEQUENCES * TOKENS) ** -0.5).astype(jnp.bfloat16)}
    for key, name in zip(kw, NAMES, strict=True):
        w = jax.random.normal(key, SHAPES[name], jnp.float32) * SHAPES[name][1] ** -0.5
        drawn[name] = (w * {"w_gate": 1.0, "w_up": bump(kh, FF, 4.0), "w_down": layers}[name]).astype(jnp.bfloat16)
    for key, name in zip(km, NAMES, strict=True):
        drawn[f"m_{name}"] = 0.1 * jax.random.normal(key, SHAPES[name], jnp.float32)
    for key, name in zip(kv, NAMES, strict=True):
        drawn[f"v_{name}"] = jax.random.uniform(key, SHAPES[name], jnp.float32, 0.005, 0.015)
    return drawn


def matmul(a, w):
    return jnp.dot(a, w, preferred_element_type=jnp.float32).astype(jnp.bfloat16)


def normed(h):
    wide = h.astype(jnp.float32)
    scale = lax.rsqrt(jnp.mean(wide**2, -1, keepdims=True) + 1e-6)
    return (wide * scale).astype(jnp.bfloat16)


def layer(h, w):
    a = normed(h)
    gate = jnp.dot(a, w["w_gate"], preferred_element_type=jnp.float32)
    up = jnp.dot(a, w["w_up"], preferred_element_type=jnp.float32)
    return h + matmul((jax.nn.silu(gate) * up).astype(jnp.bfloat16), w["w_down"])


def adamw(w, m, v, g):
    m = 0.9 * m + 0.1 * g
    v = 0.95 * v + 0.05 * g * g
    step = m * lax.rsqrt(v + 1e-8) + 0.1 * w
    return (w - 0.02 * step).astype(jnp.bfloat16), m, v


def stack(weights, h):
    return lax.scan(lambda h, w: (layer(h, w), None), h, weights)[0]


def reference(x, dy, w_gate, w_up, w_down, m_w_gate, m_w_up, m_w_down, v_w_gate, v_w_up, v_w_down):
    weights = dict(zip(NAMES, (w_gate, w_up, w_down), strict=True))

    def take(so_far, sequence):
        h, by_y = sequence
        _, back = jax.vjp(lambda w: stack(w, h), weights)
        return jax.tree.map(lambda total, term: total + term.astype(jnp.float32), so_far, back(by_y)[0]), None

    none_yet = {name: jnp.zeros(w.shape, jnp.float32) for name, w in weights.items()}
    by_weights, _ = lax.scan(take, none_yet, (x, dy))
    gradients = [by_weights[name].astype(jnp.bfloat16).astype(jnp.float32) for name in NAMES]
    new = [
        adamw(w.astype(jnp.float32), m, v, g)
        for w, m, v, g in zip((w_gate, w_up, w_down), (m_w_gate, m_w_up, m_w_down), (v_w_gate, v_w_up, v_w_down), gradients, strict=True)
    ]
    return tuple(one[which] for which in range(3) for one in new)
```

```python
import functools

import jax
import jax.numpy as jnp
from jax import lax
from jax.experimental import pallas as pl
from jax.experimental.pallas import tpu as pltpu
from jax.sharding import PartitionSpec as P

NAMES = ("w_gate", "w_up", "w_down")
MESH = pl.DeviceIdType.MESH

ROUNDS, MR = 96, 160
D0, LAG, LAGA, LAGD = 2, 2, 2, 2
RING, SLOTS = 16, 4
TICKS = ROUNDS + D0 + 3 * LAG + 3 * LAGA + max(LAGD, SLOTS)


def matmul(a, w):
    return jnp.dot(a, w, preferred_element_type=jnp.float32).astype(jnp.bfloat16)


def normed(h):
    wide = h.astype(jnp.float32)
    scale = lax.rsqrt(jnp.mean(wide**2, -1, keepdims=True) + 1e-6)
    return (wide * scale).astype(jnp.bfloat16)


def layer(h, w):
    a = normed(h)
    gate = jnp.dot(a, w["w_gate"], preferred_element_type=jnp.float32)
    up = jnp.dot(a, w["w_up"], preferred_element_type=jnp.float32)
    return h + matmul((jax.nn.silu(gate) * up).astype(jnp.bfloat16), w["w_down"])


def stack(weights, h):
    for number in range(weights["w_gate"].shape[0]):
        h = layer(h, {name: w[number] for name, w in weights.items()})
    return h


def within(r):
    return (r >= 0) & (r < ROUNDS)


def kernel(
    terms, w_g, w_u, w_d, m_g, m_u, m_d, v_g, v_u, v_d,
    news, grads, partner_terms, line_terms,
    fetched, summed, fresh, final, wb, mb, vb, wdb, mdb, vdb,
    sem_pair_s, sem_pair_r, sem_line_s, sem_line_r, sem_fetch, sem_state, sem_own, sem_ag_s, sem_ag_r, sem_agp_s, sem_agp_r,
):
    me = lax.axis_index("dp")
    z, c = lax.div(me, 2), lax.rem(me, 2)
    partner = me + 1 - 2 * c

    barrier = pltpu.get_barrier_semaphore()
    pl.semaphore_signal(barrier, inc=1, device_id={"dp": partner}, device_id_type=MESH)

    @pl.when(z > 0)
    def _():
        pl.semaphore_signal(barrier, inc=1, device_id={"dp": me - 2}, device_id_type=MESH)

    @pl.when(z < 3)
    def _():
        pl.semaphore_signal(barrier, inc=1, device_id={"dp": me + 2}, device_id_type=MESH)

    pl.semaphore_wait(barrier, 1 + (z > 0).astype(jnp.int32) + (z < 3).astype(jnp.int32))
    fetched[...] = jnp.zeros_like(fetched)

    def remote(src, dst, send, recv, dev):
        return pltpu.make_async_remote_copy(src, dst, send, recv, device_id={"dp": dev}, device_id_type=MESH)

    def pair(r):
        return remote(terms.at[r, 1 - c], partner_terms.at[r], sem_pair_s.at[lax.rem(r, SLOTS)], sem_pair_r.at[lax.rem(r, RING)], partner)

    def most(zp):
        return jnp.maximum(zp, 3 - zp)

    def fetch(i, which, src):
        return pltpu.make_async_copy(src, fetched.at[i, which], sem_fetch.at[i, which])

    class Line:
        def __init__(self, i, k):
            self.i, self.zp = i, lax.rem(z + 1 + i, 4)
            self.right = self.zp > z
            self.r = k - D0 - LAG * jnp.where(self.right, z, 3 - z)
            self.has_in = jnp.where(self.right, z > 0, z < 3)
            self.ok = within(self.r)

        def send(self, r):
            nxt = jnp.where(self.right, z + 1, z - 1)
            place = jnp.where((nxt == self.zp) & ~self.right, 4, self.zp)
            slot = lax.rem(r, SLOTS)
            return remote(
                summed.at[self.i, slot], line_terms.at[r, place],
                sem_line_s.at[self.i, slot], sem_line_r.at[place, lax.rem(r, RING)], 2 * nxt + c,
            )

        def arrival(self):
            return remote(
                summed.at[self.i, 0], line_terms.at[self.r, self.zp],
                sem_line_s.at[self.i, 0], sem_line_r.at[self.zp, lax.rem(self.r, RING)], partner,
            )

        def begin(self):
            @pl.when(self.ok)
            def _():
                fetch(self.i, 0, terms.at[self.r, c, self.zp]).start()
                fetch(self.i, 1, partner_terms.at[self.r, self.zp]).start()

            @pl.when(self.ok & self.has_in)
            def _():
                self.arrival().wait_recv()
                fetch(self.i, 2, line_terms.at[self.r, self.zp]).start()

        def finish(self):
            @pl.when(within(self.r - SLOTS))
            def _():
                self.send(self.r - SLOTS).wait_send()

            @pl.when(self.ok & self.has_in)
            def _():
                fetch(self.i, 2, line_terms.at[self.r, self.zp]).wait()

            @pl.when(self.ok)
            def _():
                fetch(self.i, 0, terms.at[self.r, c, self.zp]).wait()
                fetch(self.i, 1, partner_terms.at[self.r, self.zp]).wait()
                total = (
                    fetched[self.i, 0].astype(jnp.float32)
                    + fetched[self.i, 1].astype(jnp.float32)
                    + fetched[self.i, 2].astype(jnp.float32)
                )
                summed[self.i, lax.rem(self.r, SLOTS)] = total.astype(jnp.bfloat16)
                self.send(self.r).start()

    def state(r, go):
        kind, q, j = lax.rem(lax.div(r, 4), 3), lax.rem(r, 4), lax.rem(lax.div(r, 12), 4)
        of = 1 - lax.div(r, 48)

        @pl.when(kind == 0)
        def _():
            mine = pl.multiple_of(128 * j + 32 * q, 32)
            row = pl.multiple_of(512 * me + 128 * j + 32 * q, 32)
            go(pltpu.make_async_copy(w_d.at[of, pl.ds(row, 32)], wdb, sem_state.at[0, 0]))
            go(pltpu.make_async_copy(m_d.at[of, pl.ds(mine, 32)], mdb, sem_state.at[1, 0]))
            go(pltpu.make_async_copy(v_d.at[of, pl.ds(mine, 32)], vdb, sem_state.at[2, 0]))

        for number, (w, m, v) in ((1, (w_g, m_g, v_g)), (2, (w_u, m_u, v_u))):

            @pl.when(kind == number)
            def _(w=w, m=m, v=v):
                row = pl.multiple_of(80 * me, 16)
                for s in range(2):
                    col = pl.multiple_of(512 * (2 * q + s) + 128 * j, 128)
                    to = pl.ds(80 * s, 80)
                    go(pltpu.make_async_copy(w.at[of, pl.ds(row, 80), pl.ds(col, 128)], wb.at[to], sem_state.at[0, s]))
                    go(pltpu.make_async_copy(m.at[of, :, pl.ds(col, 128)], mb.at[to], sem_state.at[1, s]))
                    go(pltpu.make_async_copy(v.at[of, :, pl.ds(col, 128)], vb.at[to], sem_state.at[2, s]))

    def adamw(w, m, v, g):
        g = g.astype(jnp.float32)
        m = 0.9 * m + 0.1 * g
        v = 0.95 * v + 0.05 * g * g
        return (w - 0.02 * (m * lax.rsqrt(v + 1e-8) + 0.1 * w)).astype(jnp.bfloat16)

    class Own:
        def __init__(self, k):
            self.r = k - D0 - LAG * most(z)
            self.ok = within(self.r)

        def outs(self, r, go):
            slot, ring = lax.rem(r, SLOTS), lax.rem(r, RING)
            src, dst = fresh.at[slot], news.at[r, c, z]

            @pl.when(z < 3)
            def _():
                go(remote(src, dst, sem_own.at[0, slot], sem_ag_r.at[z, ring], me + 2))

            @pl.when(z > 0)
            def _():
                go(remote(src, dst, sem_own.at[1, slot], sem_ag_r.at[z, ring], me - 2))

            go(remote(src, dst, sem_own.at[2, slot], sem_agp_r.at[z, ring], partner))

        def local(self, r, go):
            slot = lax.rem(r, SLOTS)
            go(pltpu.make_async_copy(fresh.at[slot], news.at[r, c, z], sem_own.at[3, slot]))
            go(pltpu.make_async_copy(final.at[slot], grads.at[r], sem_own.at[4, slot]))

        def arrival(self, place):
            return remote(
                summed.at[0, 0], line_terms.at[self.r, place],
                sem_line_s.at[0, 0], sem_line_r.at[place, lax.rem(self.r, RING)], partner,
            )

        def begin(self):
            @pl.when(self.ok)
            def _():
                fetch(3, 0, terms.at[self.r, c, z]).start()
                fetch(3, 1, partner_terms.at[self.r, z]).start()
                state(self.r, lambda d: d.start())

            @pl.when(self.ok & (z > 0))
            def _():
                self.arrival(z).wait_recv()
                fetch(3, 2, line_terms.at[self.r, z]).start()

            @pl.when(self.ok & (z < 3))
            def _():
                self.arrival(4).wait_recv()
                fetch(3, 3, line_terms.at[self.r, 4]).start()

        def finish(self):
            @pl.when(within(self.r - SLOTS))
            def _():
                self.outs(self.r - SLOTS, lambda d: d.wait_send())
                self.local(self.r - SLOTS, lambda d: d.wait())

            @pl.when(self.ok & (z > 0))
            def _():
                fetch(3, 2, line_terms.at[self.r, z]).wait()

            @pl.when(self.ok & (z < 3))
            def _():
                fetch(3, 3, line_terms.at[self.r, 4]).wait()

            @pl.when(self.ok)
            def _():
                slot = lax.rem(self.r, SLOTS)
                kind = lax.rem(lax.div(self.r, 4), 3)
                fetch(3, 0, terms.at[self.r, c, z]).wait()
                fetch(3, 1, partner_terms.at[self.r, z]).wait()
                state(self.r, lambda d: d.wait())
                total = fetched[3, 0].astype(jnp.float32) + fetched[3, 1].astype(jnp.float32)
                total = total + fetched[3, 2].astype(jnp.float32) + fetched[3, 3].astype(jnp.float32)
                final[slot] = total.astype(jnp.bfloat16)

                @pl.when(kind == 0)
                def _():
                    for i in range(5):
                        rows, cols = pl.ds(32 * i, 32), pl.ds(128 * i, 128)
                        w = wdb[:, cols].astype(jnp.float32)
                        fresh[slot, rows] = adamw(w, mdb[:, cols], vdb[:, cols], final[slot, rows])

                @pl.when(kind != 0)
                def _():
                    fresh[slot] = adamw(wb[...].astype(jnp.float32), mb[...], vb[...], final[slot])

                self.outs(self.r, lambda d: d.start())
                self.local(self.r, lambda d: d.start())

    class Gather:
        def __init__(self, i, k):
            self.i, self.zp = i, lax.rem(z + 1 + i, 4)
            self.r = k - D0 - LAG * most(self.zp) - LAGA * jnp.abs(z - self.zp)
            self.on = jnp.where(self.zp < z, z < 3, z > 0)

        def forward(self, r):
            nxt = jnp.where(self.zp < z, z + 1, z - 1)
            at = news.at[r, c, self.zp]
            return remote(at, at, sem_ag_s.at[self.i, lax.rem(r, SLOTS)], sem_ag_r.at[self.zp, lax.rem(r, RING)], 2 * nxt + c)

        def across(self, r):
            at = news.at[r, c, self.zp]
            return remote(at, at, sem_agp_s.at[self.i, lax.rem(r, SLOTS)], sem_agp_r.at[self.zp, lax.rem(r, RING)], partner)

        def step(self):
            @pl.when(within(self.r - SLOTS) & self.on)
            def _():
                self.forward(self.r - SLOTS).wait_send()

            @pl.when(within(self.r - SLOTS))
            def _():
                self.across(self.r - SLOTS).wait_send()

            @pl.when(within(self.r))
            def _():
                self.forward(self.r).wait_recv()

            @pl.when(within(self.r) & self.on)
            def _():
                self.forward(self.r).start()

            @pl.when(within(self.r))
            def _():
                self.across(self.r).start()

    def tick(k, work=None):
        @pl.when(within(k - SLOTS))
        def _():
            pair(k - SLOTS).wait_send()

        @pl.when(within(k))
        def _():
            pair(k).start()

        @pl.when(within(k - D0))
        def _():
            pair(k - D0).wait_recv()

        own, lines = Own(k), [Line(i, k) for i in range(3)]
        for line in lines:
            line.begin()
        own.begin()
        for i in range(3):
            Gather(i, k).step()
        for zp in range(4):
            r = k - D0 - LAG * most(zp) - LAGA * jnp.abs(z - zp) - LAGD

            @pl.when(within(r))
            def _(r=r, zp=zp):
                at = news.at[r, 1 - c, zp]
                remote(at, at, sem_agp_s.at[0, 0], sem_agp_r.at[zp, lax.rem(r, RING)], partner).wait_recv()

        if work is not None:
            work()
        for line in lines:
            line.finish()
        own.finish()

    @pl.loop(0, TICKS)
    def _(k):
        tick(k)


def exchange(terms, weights, m, v):
    bf, f32, dma = jnp.bfloat16, jnp.float32, pltpu.SemaphoreType.DMA
    message = (MR, 128)
    return pl.pallas_call(
        kernel,
        name="exchange",
        out_shape=(
            jax.ShapeDtypeStruct((ROUNDS, 2, 4, *message), bf),
            jax.ShapeDtypeStruct((ROUNDS, *message), bf),
            jax.ShapeDtypeStruct((ROUNDS, 4, *message), bf),
            jax.ShapeDtypeStruct((ROUNDS, 5, *message), bf),
        ),
        in_specs=[pl.BlockSpec(memory_space=pl.ANY)] * 10,
        out_specs=[pl.BlockSpec(memory_space=pl.ANY)] * 4,
        scratch_shapes=[
            pltpu.VMEM((4, 4, *message), bf),
            pltpu.VMEM((3, SLOTS, *message), bf),
            pltpu.VMEM((SLOTS, *message), bf),
            pltpu.VMEM((SLOTS, *message), bf),
            pltpu.VMEM(message, bf), pltpu.VMEM(message, f32), pltpu.VMEM(message, f32),
            pltpu.VMEM((32, 640), bf), pltpu.VMEM((32, 640), f32), pltpu.VMEM((32, 640), f32),
            dma((SLOTS,)), dma((RING,)), dma((3, SLOTS)), dma((5, RING)), dma((4, 4)), dma((3, 2)), dma((5, SLOTS)),
            dma((3, SLOTS)), dma((4, RING)), dma((3, SLOTS)), dma((4, RING)),
        ],
        compiler_params=pltpu.CompilerParams(collective_id=0, has_side_effects=True, vmem_limit_bytes=60 * 2**20),
    )(terms, *weights, *m, *v)


def to_messages(gate, up, down):
    def wide(g):
        g = g.reshape(2, 8, 80, 4, 2, 4, 128)[::-1]
        return g.transpose(0, 5, 3, 1, 4, 2, 6).reshape(2, 4, 1, 4, 8, MR, 128)

    d = down.reshape(2, 8, 4, 4, 32, 5, 128)[::-1].transpose(0, 2, 3, 1, 5, 4, 6).reshape(2, 4, 1, 4, 8, MR, 128)
    g = jnp.concatenate([d, wide(gate), wide(up)], axis=2).reshape(ROUNDS, 4, 2, MR, 128)
    return g.transpose(0, 2, 1, 3, 4)


def from_messages(w, owners):
    w = w.reshape(2, 4, 3, 4, owners, MR, 128)[::-1]

    def wide(x):
        return x.reshape(2, 4, 4, owners, 2, 80, 128).transpose(0, 3, 5, 2, 4, 1, 6).reshape(2, owners * 80, 4096)

    down = w[:, :, 0].reshape(2, 4, 4, owners, 5, 32, 128).transpose(0, 3, 1, 2, 5, 4, 6).reshape(2, owners * 512, 640)
    return wide(w[:, :, 1]), wide(w[:, :, 2]), down


def solution(mesh):
    def step(x, dy, *arrays):
        weights, m, v = (arrays[i : i + 3] for i in (0, 3, 6))
        _, back = jax.vjp(lambda w: stack(w, x[0]), dict(zip(NAMES, weights, strict=True)))
        by_weights = back(dy[0])[0]
        terms = to_messages(*(by_weights[name] for name in NAMES))
        news, grads, _, _ = exchange(terms, weights, m, v)
        fresh = from_messages(news.transpose(0, 2, 1, 3, 4).reshape(ROUNDS, 8, MR, 128), 8)
        g = [t.astype(jnp.float32) for t in from_messages(grads, 1)]
        m = [0.9 * a + 0.1 * b for a, b in zip(m, g, strict=True)]
        v = [0.95 * a + 0.05 * b * b for a, b in zip(v, g, strict=True)]
        return (*fresh, *m, *v)

    whole, rows = P(None, None, None), P(None, "dp", None)
    return jax.shard_map(
        step,
        mesh=mesh,
        in_specs=(P(("rep", "dp"), None, None),) * 2 + (whole,) * 3 + (rows,) * 6,
        out_specs=(P("rep", None, None),) * 3 + (P("rep", "dp", None),) * 6,
        check_vma=False,
    )
```

```python
import jax
import jax.numpy as jnp
from jax import lax
from jax.experimental import pallas as pl
from jax.experimental.pallas import tpu as pltpu
from jax.sharding import PartitionSpec as P

MESH = pl.DeviceIdType.MESH
BF, F32 = jnp.bfloat16, jnp.float32

T, D, FF = 2048, 640, 4096
DEVICES, CHIPS, LANE = 8, 4, 128
TILE = DEVICES * LANE
ROWS, TALL = D // DEVICES, FF // DEVICES
PIECE, BLOCK = 512, 256

ROUNDS, MR, SUB = 96, 160, 32
PER_TILE = 12
D0, LAG, LAGF, LAGA, LAGD = 2, 2, 2, 2, 2
RING, SLOTS, KEPT = 16, 4, 12
TICKS = ROUNDS + D0 + 3 * LAG + LAGF + 2 * LAGA + max(LAGD, SLOTS)
AHEAD = 8


def normed(h):
    wide = h.astype(F32)
    scale = lax.rsqrt(jnp.mean(wide**2, -1, keepdims=True) + 1e-6)
    return (wide * scale).astype(BF)


def dot(a, b):
    return jnp.dot(a, b, preferred_element_type=F32)


def across(a, b):
    return lax.dot_general(a, b, (((1,), (1,)), ((), ())), preferred_element_type=F32)


def moments(m, v, g):
    return 0.9 * m + 0.1 * g, 0.95 * v + 0.05 * g * g


def within(r):
    return (r >= 0) & (r < ROUNDS)


def most(zp):
    return jnp.maximum(zp, CHIPS - 1 - zp)


def part(i, n):
    return pl.ds(pl.multiple_of(n * i, n), n)


def cut(i, n):
    return slice(n * i, n * i + n)


def times(n, first=0):
    return pl.loop(first, n)


def kernel(
    x, dy, w_g, w_u, w_d, m_g, m_u, m_d, v_g, v_u, v_d,
    news, grads, terms,
    mine, others, line, summed, fresh, final, wb, mb, vb, wdb, mdb, vdb,
    hv, xv, av, at, ct, ctt, wgt, wut, wdt, act, dgate, dup, dag, dau, staged, staged_d,
    sem_pair_s, sem_pair_r, sem_line_s, sem_line_r, sem_mine, sem_state, sem_own, sem_ag_s, sem_ag_r, sem_agp_s, sem_agp_r, sem_own_r,
    sem_in, sem_w, sem_st,
):
    def tile(t):
        slot, of, j = lax.rem(t, 2), lax.rem(lax.div(t, CHIPS), 2), lax.rem(t, CHIPS)
        sems = [sem_w.at[i, slot] for i in range(3)]
        for d in range(DEVICES):
            cols, to = pl.ds(pl.multiple_of(TALL * d + LANE * j, LANE), LANE), pl.ds(LANE * d, LANE)
            pltpu.make_async_copy(w_g.at[of, :, cols], wgt.at[slot, :, to], sems[0]).start()
            pltpu.make_async_copy(w_u.at[of, :, cols], wut.at[slot, :, to], sems[1]).start()
            pltpu.make_async_copy(w_d.at[of, cols], wdt.at[slot, to], sems[2]).start()

    def tile_wait(t):
        slot, all_of = lax.rem(t, 2), pl.ds(0, TILE)
        sems = [sem_w.at[i, slot] for i in range(3)]
        pltpu.make_async_copy(w_g.at[0, :, all_of], wgt.at[slot], sems[0]).wait()
        pltpu.make_async_copy(w_u.at[0, :, all_of], wut.at[slot], sems[1]).wait()
        pltpu.make_async_copy(w_d.at[0, all_of], wdt.at[slot], sems[2]).wait()

    line[...] = jnp.zeros_like(line)
    load_x, load_dy = pltpu.make_async_copy(x, xv, sem_in.at[0]), pltpu.make_async_copy(dy, ct, sem_in.at[1])
    load_x.start()
    tile(0)
    load_dy.start()
    tile(1)

    me = lax.axis_index("dp")
    z, c = lax.div(me, 2), lax.rem(me, 2)
    partner = me + 1 - 2 * c
    low, high = z > 0, z < CHIPS - 1

    barrier = pltpu.get_barrier_semaphore()

    def greet(dev):
        pl.semaphore_signal(barrier, inc=1, device_id={"dp": dev}, device_id_type=MESH)

    greet(partner)
    pl.when(low)(lambda: greet(me - 2))
    pl.when(high)(lambda: greet(me + 2))

    def remote(src, dst, send, recv, dev):
        return pltpu.make_async_remote_copy(src, dst, send, recv, device_id={"dp": dev}, device_id_type=MESH)

    def pair(r):
        slot, kept = lax.rem(r, SLOTS), lax.rem(r, KEPT)
        return remote(terms.at[r, 1 - c], others.at[kept], sem_pair_s.at[slot], sem_pair_r.at[kept], partner)

    def own_terms(r):
        kept = lax.rem(r, KEPT)
        return pltpu.make_async_copy(terms.at[r, c], mine.at[kept], sem_mine.at[kept])

    def arrival(r, place):
        ring = lax.rem(r, RING)
        return remote(summed.at[0, 0], line.at[place, ring], sem_line_s.at[0, 0], sem_line_r.at[place, ring], partner)

    def on_chip(r, zp):
        kept = lax.rem(r, KEPT)
        return mine[kept, zp].astype(F32) + others[kept, zp].astype(F32)

    class Line:
        def __init__(self, i, k):
            self.i, self.zp = i, lax.rem(z + 1 + i, CHIPS)
            self.right = self.zp > z
            self.r = k - D0 - LAG * jnp.where(self.right, z, CHIPS - 1 - z)
            self.ok = within(self.r)
            self.fed = self.ok & jnp.where(self.right, low, high)

        def send(self, r):
            nxt = jnp.where(self.right, z + 1, z - 1)
            place = jnp.where((nxt == self.zp) & ~self.right, CHIPS, self.zp)
            slot, ring = lax.rem(r, SLOTS), lax.rem(r, RING)
            return remote(summed.at[self.i, slot], line.at[place, ring], sem_line_s.at[self.i, slot], sem_line_r.at[place, ring], 2 * nxt + c)

        def step(self):
            pl.when(within(self.r - SLOTS))(lambda: self.send(self.r - SLOTS).wait_send())
            pl.when(self.fed)(lambda: arrival(self.r, self.zp).wait_recv())

            @pl.when(self.ok)
            def _():
                total = on_chip(self.r, self.zp) + line[self.zp, lax.rem(self.r, RING)].astype(F32)
                summed[self.i, lax.rem(self.r, SLOTS)] = total.astype(BF)
                self.send(self.r).start()

    def state(r, go):
        in_tile = lax.rem(r, PER_TILE)
        kind, q, t = lax.div(in_tile, CHIPS), lax.rem(r, CHIPS), lax.div(r, PER_TILE)
        of, j = 1 - lax.div(t, CHIPS), lax.rem(t, CHIPS)
        for number, (w, m, v) in enumerate(((w_g, m_g, v_g), (w_u, m_u, v_u))):

            @pl.when(kind == number)
            def _(w=w, m=m, v=v):
                rows = pl.ds(pl.multiple_of(ROWS * me, 16), ROWS)
                for s in range(2):
                    cols = pl.ds(pl.multiple_of(TALL * (2 * q + s) + LANE * j, LANE), LANE)
                    to, sems = pl.ds(ROWS * s, ROWS), [sem_state.at[i, s] for i in range(3)]
                    go(pltpu.make_async_copy(w.at[of, rows, cols], wb.at[to], sems[0]))
                    go(pltpu.make_async_copy(m.at[of, :, cols], mb.at[to], sems[1]))
                    go(pltpu.make_async_copy(v.at[of, :, cols], vb.at[to], sems[2]))

        @pl.when(kind == 2)
        def _():
            row, sems = pl.multiple_of(LANE * j + SUB * q, SUB), [sem_state.at[i, 0] for i in range(3)]
            rows = pl.ds(row, SUB)
            go(pltpu.make_async_copy(w_d.at[of, pl.ds(pl.multiple_of(TALL * me + row, SUB), SUB)], wdb, sems[0]))
            go(pltpu.make_async_copy(m_d.at[of, rows], mdb, sems[1]))
            go(pltpu.make_async_copy(v_d.at[of, rows], vdb, sems[2]))

    def adamw(w, m, v, g):
        m, v = moments(m, v, g.astype(F32))
        w = w.astype(F32)
        return (w - 0.02 * (m * lax.rsqrt(v + 1e-8) + 0.1 * w)).astype(BF)

    class Own:
        def __init__(self, k):
            self.r = k - D0 - LAG * most(z)
            self.ok = within(self.r)

        def outs(self, r, go):
            slot, ring = lax.rem(r, SLOTS), lax.rem(r, RING)
            src, dst = fresh.at[slot], news.at[r, c, z]
            pl.when(high)(lambda: go(remote(src, dst, sem_own.at[0, slot], sem_ag_r.at[z, ring], me + 2)))
            pl.when(low)(lambda: go(remote(src, dst, sem_own.at[1, slot], sem_ag_r.at[z, ring], me - 2)))
            go(remote(src, dst, sem_own.at[2, slot], sem_own_r.at[ring], partner))

        def local(self, r, go):
            slot = lax.rem(r, SLOTS)
            go(pltpu.make_async_copy(fresh.at[slot], news.at[r, c, z], sem_own.at[3, slot]))
            go(pltpu.make_async_copy(final.at[slot], grads.at[r], sem_own.at[4, slot]))

        def step(self):
            @pl.when(within(self.r - SLOTS))
            def _():
                self.outs(self.r - SLOTS, lambda d: d.wait_send())
                self.local(self.r - SLOTS, lambda d: d.wait())

            pl.when(self.ok & low)(lambda: arrival(self.r, z).wait_recv())
            pl.when(self.ok & high)(lambda: arrival(self.r, CHIPS).wait_recv())

            @pl.when(self.ok)
            def _():
                slot, ring = lax.rem(self.r, SLOTS), lax.rem(self.r, RING)
                tall = lax.rem(self.r, PER_TILE) >= 2 * CHIPS
                total = on_chip(self.r, z) + line[z, ring].astype(F32) + line[CHIPS, ring].astype(F32)
                final[slot] = total.astype(BF)
                state(self.r, lambda d: d.wait())

                @pl.when(tall)
                def _():
                    for i in range(D // LANE):
                        rows, cols = pl.ds(SUB * i, SUB), pl.ds(LANE * i, LANE)
                        fresh[slot, rows] = adamw(wdb[:, cols], mdb[:, cols], vdb[:, cols], final[slot, rows])

                @pl.when(jnp.logical_not(tall))
                def _():
                    fresh[slot] = adamw(wb[...], mb[...], vb[...], final[slot])

                self.outs(self.r, lambda d: d.start())
                self.local(self.r, lambda d: d.start())

            pl.when(within(self.r + 1))(lambda: state(self.r + 1, lambda d: d.start()))

    def sent(k, zp):
        away = jnp.abs(z - zp)
        return k - D0 - LAG * most(zp) - LAGA * away - (LAGF - LAGA) * jnp.minimum(away, 1)

    class Gather:
        def __init__(self, i, k):
            self.i, self.zp = i, lax.rem(z + 1 + i, CHIPS)
            self.r, self.up = sent(k, self.zp), self.zp < z
            self.on = jnp.where(self.up, high, low)

        def forward(self, r):
            nxt, spot = jnp.where(self.up, z + 1, z - 1), news.at[r, c, self.zp]
            return remote(spot, spot, sem_ag_s.at[self.i, lax.rem(r, SLOTS)], sem_ag_r.at[self.zp, lax.rem(r, RING)], 2 * nxt + c)

        def over(self, r):
            return bundle(r, c, self.zp, sem_agp_s.at[self.i, lax.rem(lax.div(r, SLOTS), 2)])

        def step(self):
            old, now, last = within(self.r - SLOTS), within(self.r), lax.rem(self.r, SLOTS) == SLOTS - 1
            pl.when(old & self.on)(lambda: self.forward(self.r - SLOTS).wait_send())
            pl.when(old & last)(lambda: self.over(self.r - SLOTS).wait_send())
            pl.when(now)(lambda: self.forward(self.r).wait_recv())
            pl.when(now & self.on)(lambda: self.forward(self.r).start())
            pl.when(now & last)(lambda: self.over(self.r).start())

    def bundle(r, core, zp, send):
        spot = news.at[pl.ds(r - (SLOTS - 1), SLOTS), core, zp]
        return remote(spot, spot, send, sem_agp_r.at[zp, lax.rem(lax.div(r, SLOTS), SLOTS)], partner)

    def tick(k):
        pl.when(within(k - SLOTS))(lambda: pair(k - SLOTS).wait_send())

        @pl.when(within(k))
        def _():
            pair(k).start()
            own_terms(k).start()

        @pl.when(within(k - D0))
        def _():
            pair(k - D0).wait_recv()
            own_terms(k - D0).wait()

        for i in range(CHIPS - 1):
            Line(i, k).step()
        for i in range(CHIPS - 1):
            Gather(i, k).step()
        Own(k).step()
        r = sent(k, z) - LAGD
        spot = news.at[r, 1 - c, z]
        pl.when(within(r))(lambda: remote(spot, spot, sem_agp_s.at[0, 0], sem_own_r.at[lax.rem(r, RING)], partner).wait_recv())
        for i in range(CHIPS - 1):
            zp = lax.rem(z + 1 + i, CHIPS)
            r = sent(k, zp) - LAGD
            done = within(r) & (lax.rem(r, SLOTS) == SLOTS - 1)
            pl.when(done)(lambda r=r, zp=zp: bundle(r, 1 - c, zp, sem_agp_s.at[0, 0]).wait_recv())

    load_x.wait()
    half = T // 2

    @times(T // BLOCK)
    def _(p):
        rows = part(p, BLOCK)
        av[rows] = normed(xv[rows])
        dag[rows] = jnp.zeros((BLOCK, D), F32)

    def hidden(i):
        slot, rows = lax.rem(lax.div(i, 2), 2), part(lax.rem(i, 2), half)
        a = av[rows]
        for n in range(TILE // PIECE):
            cols = pl.ds(PIECE * n, PIECE)
            gate, up = dot(a, wgt[slot, :, cols]), dot(a, wut[slot, :, cols])
            act[rows, cols] = (gate * jax.nn.sigmoid(gate) * up).astype(BF)

    def turn(i):
        rows = part(i, BLOCK)
        ctt[:, rows] = ct[rows].T

    def back(i):
        slot, rows = lax.rem(lax.div(i, 2), 2), part(lax.rem(i, 2), half)
        dag[rows] = dag[rows] + dot(act[rows], wdt[slot])

    tile_wait(0)
    hidden(0)
    load_dy.wait()
    turn(0)

    @times(2 * CHIPS, first=1)
    def _(i):
        first, t = lax.rem(i, 2) == 0, lax.div(i, 2)
        pl.when(first)(lambda: tile_wait(t))
        pl.when(jnp.logical_not(first) & (t > 0))(lambda: tile(t + 1))
        back(i - 1)
        hidden(i)
        turn(i)

    back(2 * CHIPS - 1)

    @times(T // BLOCK)
    def _(p):
        rows = part(p, BLOCK)
        h = xv[rows] + dag[rows].astype(BF)
        a = normed(h)
        hv[rows], av[rows], at[:, rows] = h, a, a.T
        dag[rows] = dau[rows] = jnp.zeros((BLOCK, D), F32)

    def next_layer(q):
        @times(PIECE // BLOCK)
        def _(i):
            rows = part(PIECE // BLOCK * q + i, BLOCK)
            da = (dag[rows].astype(BF) + dau[rows].astype(BF)).astype(F32)
            wide = hv[rows].astype(F32)
            mean = jnp.mean(wide * wide, -1, keepdims=True) + 1e-6
            scale = lax.rsqrt(mean)
            along = jnp.sum(da * wide, -1, keepdims=True) * (-scale / (D * mean))
            by = ct[rows] + (da * scale + wide * along).astype(BF)
            a = normed(xv[rows])
            ct[rows], ctt[:, rows], av[rows], at[:, rows] = by, by.T, a, a.T

    def tokens(slot, p):
        rows = part(p, PIECE)
        a, by = av[rows], ct[rows]
        for n in range(TILE // PIECE):
            cols = pl.ds(PIECE * n, PIECE)
            gate, up = dot(a, wgt[slot, :, cols]), dot(a, wut[slot, :, cols])
            dact = across(by, wdt[slot, cols]).astype(BF).astype(F32)
            sig = jax.nn.sigmoid(gate)
            silu = gate * sig
            act[rows, cols] = (silu * up).astype(BF)
            dup[rows, cols] = (dact * silu).astype(BF)
            dgate[rows, cols] = (dact * up * (sig + silu * (1.0 - sig))).astype(BF)

    def put(slot, r):
        return pltpu.make_async_copy(staged.at[slot], terms.at[r], sem_st.at[slot])

    def put_d(t, go):
        for q in range(CHIPS):
            go(pltpu.make_async_copy(staged_d.at[q], terms.at[PER_TILE * t + 2 * CHIPS + q], sem_st.at[2 + q]))

    def wide_terms(by, slot, q, r):
        g = dot(at[...], by[:, part(q, BLOCK)]).astype(BF)
        for d in range(DEVICES):
            for s in range(2):
                staged[slot, d % 2, d // 2, cut(s, ROWS)] = g[cut(d, ROWS), cut(s, LANE)]
        put(slot, r).start()

    def down_terms(i):
        g = dot(ctt[...], act[:, part(i, BLOCK)]).T.astype(BF)
        for o in range(2):
            for q in range(CHIPS):
                for s in range(D // LANE):
                    staged_d[q, o, i, cut(s, SUB)] = g[cut(CHIPS * o + q, SUB), cut(s, LANE)]

    def by_normed(to, by, w, slot, p):
        rows = part(p, PIECE)
        to[rows] = to[rows] + across(by[rows], w[slot])

    pl.semaphore_wait(barrier, 1 + low.astype(jnp.int32) + high.astype(jnp.int32))

    @times(TICKS + AHEAD)
    def _(n):
        q, phase, t = lax.rem(n, CHIPS), lax.div(lax.rem(n, PER_TILE), CHIPS), lax.div(n, PER_TILE)
        slot, busy = lax.rem(t, 2), n < ROUNDS

        @pl.when(busy & (phase == 0) & (q == 0))
        def _():
            tile_wait(t)
            pl.when(n < ROUNDS - PER_TILE)(lambda: tile(t + CHIPS + 1))

        pl.when((n > 0) & (n <= ROUNDS) & (lax.rem(n - 1, PER_TILE) >= CHIPS))(lambda: put(lax.rem(n - 1, 2), n - 1 - CHIPS).wait())
        pl.when((phase == 0) & (q == 2) & (n >= PER_TILE) & (n < ROUNDS + PER_TILE))(lambda: put_d(t - 1, lambda d: d.wait()))

        def work():
            @pl.when(busy & (phase == 0))
            def _():
                pl.when(t == CHIPS)(lambda: next_layer(q))
                tokens(slot, q)

            @pl.when(busy & (phase == 1))
            def _():
                wide_terms(dgate, lax.rem(n, 2), q, n - CHIPS)
                pl.when((t > 0) & (t < CHIPS))(lambda: by_normed(dag, dgate, wgt, slot, q))

            @pl.when(busy & (phase == 2))
            def _():
                wide_terms(dup, lax.rem(n, 2), q, n - CHIPS)
                down_terms(q)
                pl.when(t == 0)(lambda: by_normed(dag, dgate, wgt, slot, q))
                pl.when(t < CHIPS)(lambda: by_normed(dau, dup, wut, slot, q))
                pl.when(q == CHIPS - 1)(lambda: put_d(t, lambda d: d.start()))

        tick(n - AHEAD)
        work()


def backward(x, dy, weights, m, v):
    def dma(*shape):
        return pltpu.SemaphoreType.DMA(shape)

    def bf(*shape):
        return pltpu.VMEM(shape, BF)

    def f32(*shape):
        return pltpu.VMEM(shape, F32)

    message = (MR, LANE)
    outs = ((2, CHIPS, *message), message, (2, CHIPS, *message))
    anywhere = pl.BlockSpec(memory_space=pl.ANY)
    return pl.pallas_call(
        kernel,
        name="backward",
        out_shape=[jax.ShapeDtypeStruct((ROUNDS, *s), BF) for s in outs],
        in_specs=[anywhere] * 11,
        out_specs=[anywhere] * len(outs),
        scratch_shapes=[
            bf(KEPT, CHIPS, *message), bf(KEPT, CHIPS, *message), bf(CHIPS + 1, RING, *message), bf(3, SLOTS, *message), bf(SLOTS, *message), bf(SLOTS, *message),
            bf(*message), f32(*message), f32(*message), bf(SUB, D), f32(SUB, D), f32(SUB, D),
            bf(T, D), bf(T, D), bf(T, D), bf(D, T), bf(T, D), bf(D, T),
            bf(2, D, TILE), bf(2, D, TILE), bf(2, TILE, D),
            bf(T, TILE), bf(T, TILE), bf(T, TILE), f32(T, D), f32(T, D),
            bf(2, 2, CHIPS, *message), bf(CHIPS, 2, CHIPS, *message),
            dma(SLOTS), dma(KEPT), dma(3, SLOTS), dma(CHIPS + 1, RING), dma(KEPT), dma(3, 2), dma(5, SLOTS),
            dma(3, SLOTS), dma(CHIPS, RING), dma(3, 2), dma(CHIPS, SLOTS), dma(RING),
            dma(2), dma(3, 2), dma(2 + CHIPS),
        ],
        compiler_params=pltpu.CompilerParams(collective_id=0, has_side_effects=True, vmem_limit_bytes=67_043_328),
    )(x, dy, *weights, *m, *v)


DEPTH, STORES = 4, 3


def finish_kernel(*refs):
    def three(first):
        return refs[first : first + 3]

    news, grads, m, v = refs[0], refs[1], three(2), three(5)
    w_out, m_out, v_out = three(8), three(11), three(14)
    new_in, grad_in, m_in, v_in = three(17), three(20), three(23), three(26)
    w_to, m_to, v_to = three(29), three(32), three(35)
    sem_in, sem_out = refs[38:]
    steps = 2 * DEVICES

    def where(i):
        n, d = lax.div(i, DEVICES), lax.rem(i, DEVICES)
        wide, tall = pl.ds(pl.multiple_of(PIECE * d, PIECE), PIECE), pl.ds(pl.multiple_of(2 * SUB * d, 2 * SUB), 2 * SUB)
        return n, d, [(n, slice(None), wide)] * 2 + [(n, tall)]

    def loads(i, go):
        slot = lax.rem(i, DEPTH)
        n, d, states = where(i)
        core, chip, of = lax.rem(d, 2), lax.div(d, 2), 1 - n
        for kind in range(3):
            if kind < 2:
                grad = grads.at[of, :, kind, chip]
            else:
                grad = grads.at[of, chip, kind, pl.ds(2 * core, 2)]
            pairs = (
                (news.at[of, :, kind, :, core, chip], new_in[kind]),
                (grad, grad_in[kind]),
                (m[kind].at[states[kind]], m_in[kind]),
                (v[kind].at[states[kind]], v_in[kind]),
            )
            for number, (src, dst) in enumerate(pairs):
                go(pltpu.make_async_copy(src, dst.at[slot], sem_in.at[slot, kind, number]))

    def stores(i, go):
        slot = lax.rem(i, STORES)
        n, d, states = where(i)
        rows, tall = pl.ds(pl.multiple_of(ROWS * d, 16), ROWS), pl.ds(pl.multiple_of(TALL * d, TALL), TALL)
        for kind in range(3):
            pairs = (
                (w_to[kind], w_out[kind].at[n, rows if kind < 2 else tall]),
                (m_to[kind], m_out[kind].at[states[kind]]),
                (v_to[kind], v_out[kind].at[states[kind]]),
            )
            for number, (src, dst) in enumerate(pairs):
                go(pltpu.make_async_copy(src.at[slot], dst, sem_out.at[slot, kind, number]))

    for first in range(DEPTH):
        loads(first, lambda d: d.start())

    @times(steps)
    def _(i):
        slot, to, s = lax.rem(i, DEPTH), lax.rem(i, STORES), lax.rem(i, 2)
        loads(i, lambda d: d.wait())
        pl.when(i >= STORES)(lambda: stores(i - STORES, lambda d: d.wait()))

        def step(kind, rows, cols, g):
            old_m, old_v = m_in[kind][slot, rows, cols], v_in[kind][slot, rows, cols]
            m_to[kind][to, rows, cols], v_to[kind][to, rows, cols] = moments(old_m, old_v, g.astype(F32))

        for kind in range(2):
            for j in range(CHIPS):
                for q in range(CHIPS):
                    for half in range(2):
                        w_to[kind][to, :, cut(4 * (2 * q + half) + j, LANE)] = new_in[kind][slot, j, q, cut(half, ROWS)]
                step(kind, slice(ROWS), cut(j, LANE), grad_in[kind][slot, j, part(s, ROWS)])
        for number in range(D // LANE):
            for j in range(CHIPS):
                for q in range(CHIPS):
                    w_to[2][to, cut(CHIPS * j + q, SUB), cut(number, LANE)] = new_in[2][slot, j, q, cut(number, SUB)]
            for q in range(2):
                step(2, cut(q, SUB), cut(number, LANE), grad_in[2][slot, q, cut(number, SUB)])
        stores(i, lambda d: d.start())
        pl.when(i < steps - DEPTH)(lambda: loads(i + DEPTH, lambda d: d.start()))

    for last in range(STORES):
        stores(steps - STORES + last, lambda d: d.wait())


def finish(news, grads, m, v):
    shape = (2, CHIPS, 3, CHIPS)
    news, grads = news.reshape(*shape, 2, CHIPS, MR, LANE), grads.reshape(*shape, MR, LANE)
    anywhere = pl.BlockSpec(memory_space=pl.ANY)
    blocks = [(ROWS, PIECE), (ROWS, PIECE), (2 * SUB, D)]
    states = [jax.ShapeDtypeStruct(a.shape, F32) for a in m]
    return pl.pallas_call(
        finish_kernel,
        name="finish",
        out_shape=[*[jax.ShapeDtypeStruct((2, D, FF), BF)] * 2, jax.ShapeDtypeStruct((2, FF, D), BF), *states * 2],
        in_specs=[anywhere] * 8,
        out_specs=[anywhere] * 9,
        scratch_shapes=[
            *[pltpu.VMEM((DEPTH, CHIPS, CHIPS, MR, LANE), BF)] * 3,
            *[pltpu.VMEM((DEPTH, n, MR, LANE), BF) for n in (CHIPS, CHIPS, 2)],
            *[pltpu.VMEM((DEPTH, *b), F32) for b in blocks * 2],
            *[pltpu.VMEM((STORES, *b), BF) for b in ((ROWS, FF), (ROWS, FF), (TALL, D))],
            *[pltpu.VMEM((STORES, *b), F32) for b in blocks * 2],
            pltpu.SemaphoreType.DMA((DEPTH, 3, 4)), pltpu.SemaphoreType.DMA((STORES, 3, 3)),
        ],
        compiler_params=pltpu.CompilerParams(vmem_limit_bytes=60 * 2**20),
    )(news, grads, *m, *v)


def solution(mesh):
    def step(x, dy, *arrays):
        weights, m, v = (arrays[i : i + 3] for i in (0, 3, 6))
        news, grads, *_ = backward(x[0], dy[0], weights, m, v)
        return tuple(finish(news, grads, m, v))

    by_device, whole, rows = P(("rep", "dp")), P(), P(None, "dp")
    return jax.shard_map(
        step,
        mesh=mesh,
        in_specs=(by_device,) * 2 + (whole,) * 3 + (rows,) * 6,
        out_specs=(P("rep"),) * 3 + (P("rep", "dp"),) * 6,
        check_vma=False,
    )
```

```python
import jax
import jax.numpy as jnp
from jax import lax
from jax.experimental import pallas as pl
from jax.experimental.pallas import tpu as pltpu
from jax.sharding import PartitionSpec as P

MESH = pl.DeviceIdType.MESH
BF, F32 = jnp.bfloat16, jnp.float32

T, D, FF = 2048, 640, 4096
DEVICES, CHIPS, LANE = 8, 4, 128
TILE = DEVICES * LANE
ROWS, TALL = D // DEVICES, FF // DEVICES
PIECE, BLOCK = 512, 256

ROUNDS, MR, SUB = 96, 160, 32
PER_TILE = 12
D0, LAG, LAGF, LAGA, LAGD = 2, 2, 3, 3, 2
RING, SLOTS, KEPT = 16, 4, 12
TICKS = ROUNDS + D0 + 3 * LAG + LAGF + 2 * LAGA + max(LAGD, SLOTS)
AHEAD = 6


def normed(h):
    wide = h.astype(F32)
    scale = lax.rsqrt(jnp.mean(wide**2, -1, keepdims=True) + 1e-6)
    return (wide * scale).astype(BF)


def dot(a, b):
    return jnp.dot(a, b, preferred_element_type=F32)


def across(a, b):
    return lax.dot_general(a, b, (((1,), (1,)), ((), ())), preferred_element_type=F32)


def moments(m, v, g):
    return 0.9 * m + 0.1 * g, 0.95 * v + 0.05 * g * g


def within(r):
    return (r >= 0) & (r < ROUNDS)


def stage(n):
    t = lax.div(n, PER_TILE)
    return t, lax.rem(n, PER_TILE), lax.rem(t, CHIPS) == 0


def plan(r):
    t, i, early = stage(r + CHIPS)
    late = i - CHIPS
    kind = jnp.where(early, jnp.where(late < 0, 2, lax.rem(late, 2)), lax.rem(i, 3))
    q = jnp.where(early, jnp.where(late < 0, i, lax.div(late, 2)), lax.div(i, 3))
    t = t - lax.div(kind, 2)
    return PER_TILE * t + CHIPS * kind + q, t, kind, q


def ends_kind(r):
    _, i, early = stage(r + CHIPS)
    return jnp.where(early, (i == 3) | (i >= PER_TILE - 2), i >= PER_TILE - 3)


def most(zp):
    return jnp.maximum(zp, CHIPS - 1 - zp)


def part(i, n):
    return pl.ds(pl.multiple_of(n * i, n), n)


def cut(i, n):
    return slice(n * i, n * i + n)


def times(n, first=0):
    return pl.loop(first, n)


def kernel(
    x, dy, w_g, w_u, w_d, m_g, m_u, m_d, v_g, v_u, v_d,
    news, grads, terms,
    mine, others, line, summed, fresh, final, wb, mb, vb, wdb, mdb, vdb,
    hv, xv, av, at, ct, ctt, wgt, wut, wdt, act, dgate, dup, dag, dau, staged, staged_d,
    sem_pair_s, sem_pair_r, sem_line_s, sem_line_r, sem_mine, sem_state, sem_own, sem_ag_s, sem_ag_r, sem_agp_s, sem_agp_r, sem_own_r,
    sem_in, sem_w, sem_st,
):
    def tile(t):
        slot, of, j = lax.rem(t, 2), lax.rem(lax.div(t, CHIPS), 2), lax.rem(t, CHIPS)
        sems = [sem_w.at[i, slot] for i in range(3)]
        for d in range(DEVICES):
            cols, to = pl.ds(pl.multiple_of(TALL * d + LANE * j, LANE), LANE), pl.ds(LANE * d, LANE)
            pltpu.make_async_copy(w_g.at[of, :, cols], wgt.at[slot, :, to], sems[0]).start()
            pltpu.make_async_copy(w_u.at[of, :, cols], wut.at[slot, :, to], sems[1]).start()
            pltpu.make_async_copy(w_d.at[of, cols], wdt.at[slot, to], sems[2]).start()

    def tile_wait(t):
        slot, all_of = lax.rem(t, 2), pl.ds(0, TILE)
        sems = [sem_w.at[i, slot] for i in range(3)]
        pltpu.make_async_copy(w_g.at[0, :, all_of], wgt.at[slot], sems[0]).wait()
        pltpu.make_async_copy(w_u.at[0, :, all_of], wut.at[slot], sems[1]).wait()
        pltpu.make_async_copy(w_d.at[0, all_of], wdt.at[slot], sems[2]).wait()

    line[...] = jnp.zeros_like(line)
    upper, lower = pl.ds(0, T // 2), pl.ds(T // 2, T // 2)
    load_x, load_more = (pltpu.make_async_copy(x.at[rows], xv.at[rows], sem_in.at[i]) for i, rows in enumerate((upper, lower)))
    load_dy = pltpu.make_async_copy(dy, ct, sem_in.at[2])
    load_x.start()
    tile(0)
    load_more.start()
    load_dy.start()
    tile(1)

    me = lax.axis_index("dp")
    z, c = lax.div(me, 2), lax.rem(me, 2)
    partner = me + 1 - 2 * c
    low, high = z > 0, z < CHIPS - 1

    barrier = pltpu.get_barrier_semaphore()

    def greet(dev):
        pl.semaphore_signal(barrier, inc=1, device_id={"dp": dev}, device_id_type=MESH)

    greet(partner)
    pl.when(low)(lambda: greet(me - 2))
    pl.when(high)(lambda: greet(me + 2))

    def remote(src, dst, send, recv, dev):
        return pltpu.make_async_remote_copy(src, dst, send, recv, device_id={"dp": dev}, device_id_type=MESH)

    def pair(r, at_round=0):
        slot, kept = lax.rem(r, SLOTS), lax.rem(r, KEPT)
        return remote(terms.at[at_round, 1 - c], others.at[kept], sem_pair_s.at[slot], sem_pair_r.at[kept], partner)

    def own_terms(r, at_round=0):
        kept = lax.rem(r, KEPT)
        return pltpu.make_async_copy(terms.at[at_round, c], mine.at[kept], sem_mine.at[kept])

    def arrival(r, place):
        ring = lax.rem(r, RING)
        return remote(summed.at[0, 0], line.at[place, ring], sem_line_s.at[0, 0], sem_line_r.at[place, ring], partner)

    def on_chip(r, zp):
        kept = lax.rem(r, KEPT)
        return mine[kept, zp].astype(F32) + others[kept, zp].astype(F32)

    class Line:
        def __init__(self, i, k):
            self.i, self.zp = i, lax.rem(z + 1 + i, CHIPS)
            self.right = self.zp > z
            self.r = k - D0 - LAG * jnp.where(self.right, z, CHIPS - 1 - z)
            self.ok = within(self.r)
            self.fed = self.ok & jnp.where(self.right, low, high)

        def send(self, r):
            nxt = jnp.where(self.right, z + 1, z - 1)
            place = jnp.where((nxt == self.zp) & ~self.right, CHIPS, self.zp)
            slot, ring = lax.rem(r, SLOTS), lax.rem(r, RING)
            return remote(summed.at[self.i, slot], line.at[place, ring], sem_line_s.at[self.i, slot], sem_line_r.at[place, ring], 2 * nxt + c)

        def step(self):
            pl.when(within(self.r - SLOTS))(lambda: self.send(self.r - SLOTS).wait_send())
            pl.when(self.fed)(lambda: arrival(self.r, self.zp).wait_recv())

            @pl.when(self.ok)
            def _():
                total = on_chip(self.r, self.zp) + line[self.zp, lax.rem(self.r, RING)].astype(F32)
                summed[self.i, lax.rem(self.r, SLOTS)] = total.astype(BF)
                self.send(self.r).start()

    def state(r, go):
        _, t, kind, q = plan(r)
        of, j = 1 - lax.div(t, CHIPS), lax.rem(t, CHIPS)
        for number, (w, m, v) in enumerate(((w_g, m_g, v_g), (w_u, m_u, v_u))):

            @pl.when(kind == number)
            def _(w=w, m=m, v=v):
                rows = pl.ds(pl.multiple_of(ROWS * me, 16), ROWS)
                for s in range(2):
                    cols = pl.ds(pl.multiple_of(TALL * (2 * q + s) + LANE * j, LANE), LANE)
                    to, sems = pl.ds(ROWS * s, ROWS), [sem_state.at[i, s] for i in range(3)]
                    go(pltpu.make_async_copy(w.at[of, rows, cols], wb.at[to], sems[0]))
                    go(pltpu.make_async_copy(m.at[of, :, cols], mb.at[to], sems[1]))
                    go(pltpu.make_async_copy(v.at[of, :, cols], vb.at[to], sems[2]))

        @pl.when(kind == 2)
        def _():
            row, sems = pl.multiple_of(LANE * j + SUB * q, SUB), [sem_state.at[i, 0] for i in range(3)]
            rows = pl.ds(row, SUB)
            go(pltpu.make_async_copy(w_d.at[of, pl.ds(pl.multiple_of(TALL * me + row, SUB), SUB)], wdb, sems[0]))
            go(pltpu.make_async_copy(m_d.at[of, rows], mdb, sems[1]))
            go(pltpu.make_async_copy(v_d.at[of, rows], vdb, sems[2]))

    def adamw(w, m, v, g):
        m, v = moments(m, v, g.astype(F32))
        w = w.astype(F32)
        return (w - 0.02 * (m * lax.rsqrt(v + 1e-8) + 0.1 * w)).astype(BF)

    class Own:
        def __init__(self, k):
            self.r = k - D0 - LAG * most(z)
            self.ok = within(self.r)

        def outs(self, r, go, at_round=0):
            slot, ring = lax.rem(r, SLOTS), lax.rem(r, RING)
            src, dst = fresh.at[slot], news.at[at_round, c, z]
            pl.when(high)(lambda: go(remote(src, dst, sem_own.at[0, slot], sem_ag_r.at[z, ring], me + 2)))
            pl.when(low)(lambda: go(remote(src, dst, sem_own.at[1, slot], sem_ag_r.at[z, ring], me - 2)))
            go(remote(src, dst, sem_own.at[2, slot], sem_own_r.at[ring], partner))

        def local(self, r, go, at_round=0):
            slot = lax.rem(r, SLOTS)
            go(pltpu.make_async_copy(fresh.at[slot], news.at[at_round, c, z], sem_own.at[3, slot]))
            go(pltpu.make_async_copy(final.at[slot], grads.at[at_round], sem_own.at[4, slot]))

        def step(self):
            @pl.when(within(self.r - SLOTS))
            def _():
                self.outs(self.r - SLOTS, lambda d: d.wait_send())
                self.local(self.r - SLOTS, lambda d: d.wait())

            pl.when(self.ok & low)(lambda: arrival(self.r, z).wait_recv())
            pl.when(self.ok & high)(lambda: arrival(self.r, CHIPS).wait_recv())

            @pl.when(self.ok)
            def _():
                slot, ring = lax.rem(self.r, SLOTS), lax.rem(self.r, RING)
                at_round, _, kind, _ = plan(self.r)
                total = on_chip(self.r, z) + line[z, ring].astype(F32) + line[CHIPS, ring].astype(F32)
                final[slot] = total.astype(BF)
                state(self.r, lambda d: d.wait())

                @pl.when(kind == 2)
                def _():
                    for i in range(D // LANE):
                        rows, cols = pl.ds(SUB * i, SUB), pl.ds(LANE * i, LANE)
                        fresh[slot, rows] = adamw(wdb[:, cols], mdb[:, cols], vdb[:, cols], final[slot, rows])

                @pl.when(kind < 2)
                def _():
                    fresh[slot] = adamw(wb[...], mb[...], vb[...], final[slot])

                self.outs(self.r, lambda d: d.start(), at_round)
                self.local(self.r, lambda d: d.start(), at_round)

            pl.when(within(self.r + 1))(lambda: state(self.r + 1, lambda d: d.start()))

    def sent(k, zp):
        away = jnp.abs(z - zp)
        return k - D0 - LAG * most(zp) - LAGA * away - (LAGF - LAGA) * jnp.minimum(away, 1)

    class Gather:
        def __init__(self, i, k):
            self.i, self.zp = i, lax.rem(z + 1 + i, CHIPS)
            self.r, self.up = sent(k, self.zp), self.zp < z
            self.on = jnp.where(self.up, high, low)

        def forward(self, r, at_round=0):
            nxt, spot = jnp.where(self.up, z + 1, z - 1), news.at[at_round, c, self.zp]
            return remote(spot, spot, sem_ag_s.at[self.i, lax.rem(r, SLOTS)], sem_ag_r.at[self.zp, lax.rem(r, RING)], 2 * nxt + c)

        def over(self, r, at_round=CHIPS - 1):
            return bundle(r, at_round, c, self.zp, sem_agp_s.at[self.i, lax.rem(r, SLOTS)])

        def step(self):
            r, old, now = self.r, within(self.r - SLOTS), within(self.r)
            pl.when(old & self.on)(lambda: self.forward(r - SLOTS).wait_send())
            pl.when(old & ends_kind(r - SLOTS))(lambda: self.over(r - SLOTS).wait_send())

            @pl.when(now)
            def _():
                self.forward(r).wait_recv()
                at_round, _, _, q = plan(r)
                pl.when(self.on)(lambda: self.forward(r, at_round).start())
                pl.when(q == CHIPS - 1)(lambda: self.over(r, at_round).start())

    def bundle(r, at_round, core, zp, send):
        spot = news.at[pl.ds(at_round - (CHIPS - 1), CHIPS), core, zp]
        return remote(spot, spot, send, sem_agp_r.at[zp, lax.rem(r, RING)], partner)

    def tick(k):
        pl.when(within(k - SLOTS))(lambda: pair(k - SLOTS).wait_send())

        @pl.when(within(k - D0))
        def _():
            pair(k - D0).wait_recv()
            own_terms(k - D0).wait()

        for i in range(CHIPS - 1):
            Line(i, k).step()
        for i in range(CHIPS - 1):
            Gather(i, k).step()
        Own(k).step()
        r = sent(k, z) - LAGD
        spot = news.at[0, 1 - c, z]
        pl.when(within(r))(lambda: remote(spot, spot, sem_agp_s.at[0, 0], sem_own_r.at[lax.rem(r, RING)], partner).wait_recv())
        for i in range(CHIPS - 1):
            zp = lax.rem(z + 1 + i, CHIPS)
            r = sent(k, zp) - LAGD
            done = within(r) & ends_kind(r)
            pl.when(done)(lambda r=r, zp=zp: bundle(r, CHIPS - 1, 1 - c, zp, sem_agp_s.at[0, 0]).wait_recv())

    def begin_round(k):
        @pl.when(within(k))
        def _():
            at_round = plan(k)[0]
            pair(k, at_round).start()
            own_terms(k, at_round).start()

    half = T // 2
    blocks = half // BLOCK

    def enter(p):
        rows = part(p, BLOCK)
        av[rows] = normed(xv[rows])
        dag[rows] = jnp.zeros((BLOCK, D), F32)

    def hidden(i):
        slot, rows = lax.rem(lax.div(i, 2), 2), part(lax.rem(i, 2), half)
        a = av[rows]
        for n in range(TILE // PIECE):
            cols = pl.ds(PIECE * n, PIECE)
            gate, up = dot(a, wgt[slot, :, cols]), dot(a, wut[slot, :, cols])
            act[rows, cols] = (gate * jax.nn.sigmoid(gate) * up).astype(BF)

    def turn(i):
        rows = part(i, BLOCK)
        ctt[:, rows] = ct[rows].T

    def back(i):
        slot, rows = lax.rem(lax.div(i, 2), 2), part(lax.rem(i, 2), half)
        dag[rows] = dag[rows] + dot(act[rows], wdt[slot])

    def leave(p):
        rows = part(p, BLOCK)
        h = xv[rows] + dag[rows].astype(BF)
        a = normed(h)
        hv[rows], av[rows], at[:, rows] = h, a, a.T
        dag[rows] = dau[rows] = jnp.zeros((BLOCK, D), F32)

    load_x.wait()
    times(blocks)(enter)
    tile_wait(0)
    load_more.wait()
    hidden(0)
    for p in range(blocks):
        enter(blocks + p)
    load_dy.wait()
    turn(0)

    @times(2 * CHIPS, first=1)
    def _(i):
        first, t = lax.rem(i, 2) == 0, lax.div(i, 2)
        pl.when(first)(lambda: tile_wait(t))
        pl.when(jnp.logical_not(first) & (t > 0))(lambda: tile(t + 1))
        back(i - 1)
        hidden(i)
        turn(i)

    back(2 * CHIPS - 1)
    for p in range(blocks):
        leave(p)
    times(2 * blocks, first=blocks)(leave)

    def next_layer(q):
        @times(PIECE // BLOCK)
        def _(i):
            rows = part(PIECE // BLOCK * q + i, BLOCK)
            da = (dag[rows].astype(BF) + dau[rows].astype(BF)).astype(F32)
            wide = hv[rows].astype(F32)
            mean = jnp.mean(wide * wide, -1, keepdims=True) + 1e-6
            scale = lax.rsqrt(mean)
            along = jnp.sum(da * wide, -1, keepdims=True) * (-scale / (D * mean))
            by = ct[rows] + (da * scale + wide * along).astype(BF)
            a = normed(xv[rows])
            ct[rows], ctt[:, rows], av[rows], at[:, rows] = by, by.T, a, a.T

    def tokens(slot, q):
        cols = part(q, BLOCK)

        @times(2)
        def _(p):
            rows = part(p, half)
            a, by = av[rows], ct[rows]
            gate, up = dot(a, wgt[slot, :, cols]), dot(a, wut[slot, :, cols])
            dact = across(by, wdt[slot, cols]).astype(BF).astype(F32)
            sig = jax.nn.sigmoid(gate)
            silu = gate * sig
            act[rows, cols] = (silu * up).astype(BF)
            dup[rows, cols] = (dact * silu).astype(BF)
            dgate[rows, cols] = (dact * up * (sig + silu * (1.0 - sig))).astype(BF)

    def put(slot, r):
        return pltpu.make_async_copy(staged.at[slot], terms.at[r], sem_st.at[slot])

    def put_d(t, go):
        for q in range(CHIPS):
            go(pltpu.make_async_copy(staged_d.at[q], terms.at[PER_TILE * t + 2 * CHIPS + q], sem_st.at[2 + q]))

    def wide_terms(by, kind, t, q):
        g = dot(at[...], by[:, part(q, BLOCK)]).astype(BF)
        for d in range(DEVICES):
            for s in range(2):
                staged[kind, d % 2, d // 2, cut(s, ROWS)] = g[cut(d, ROWS), cut(s, LANE)]
        put(kind, PER_TILE * t + CHIPS * kind + q).start()

    def down_terms(i):
        g = dot(ctt[...], act[:, part(i, BLOCK)]).T.astype(BF)
        for o in range(2):
            for q in range(CHIPS):
                for s in range(D // LANE):
                    staged_d[q, o, i, cut(s, SUB)] = g[cut(CHIPS * o + q, SUB), cut(s, LANE)]

    def by_normed(slot, p, side):
        rows, cols = part(p, PIECE), part(side, PIECE)
        for to, by, w in ((dag, dgate, wgt), (dau, dup, wut)):
            to[rows] = to[rows] + across(by[rows, cols], w[slot, :, cols])

    pl.semaphore_wait(barrier, 1 + low.astype(jnp.int32) + high.astype(jnp.int32))

    def makes(n):
        _, i, early = stage(n)
        odd = (i > CHIPS) & (lax.rem(i, 2) == 1)
        real = (n >= CHIPS) & (n < ROUNDS)
        return real & jnp.where(early, odd, lax.rem(i, 3) == 1), real & jnp.where(early, odd, lax.rem(i, 3) == 2)

    @times(TICKS + AHEAD, first=CHIPS)
    def _(n):
        t, i, early = stage(n)
        slot, busy = lax.rem(t, 2), n < ROUNDS
        q = jnp.where(early, lax.div(jnp.maximum(i - CHIPS, 0), 2), lax.div(i, 3))
        of_three = lax.rem(i, 3)
        starts = jnp.where(early, (i >= CHIPS) & (lax.rem(i, 2) == 0), of_three == 0)
        gate_terms, up_terms = makes(n)

        @pl.when(busy & starts & (q == 0))
        def _():
            tile_wait(t)

        pl.when((i == CHIPS + 2) & (n < ROUNDS - PER_TILE))(lambda: tile(t + CHIPS + 1))

        tick(n - AHEAD)

        for number, made in enumerate(makes(n - 1)):
            pl.when(made)(lambda number=number: put(number, 0).wait())
        pl.when((i == 1) & (n >= PER_TILE) & (n < ROUNDS + PER_TILE))(lambda: put_d(0, lambda d: d.wait()))
        begin_round(n - AHEAD)

        first_tile, turning = t == 0, t == CHIPS
        between = (t > 0) & (t < CHIPS) & (of_three > 0)
        back_on = first_tile & (i >= 2 * CHIPS) | turning & (i < CHIPS) | between
        before = turning | ~first_tile & (q < 2)
        place = jnp.where(first_tile, i - 2 * CHIPS, jnp.where(turning, i, 2 * lax.rem(q, 2) + of_three - 1))
        pl.when(back_on)(lambda: by_normed(jnp.where(before, 1 - slot, slot), place, before.astype(jnp.int32)))
        pl.when(turning & (i < CHIPS))(lambda: next_layer(i))
        pl.when(busy & starts)(lambda: tokens(slot, q))
        pl.when(gate_terms)(lambda: wide_terms(dgate, 0, t, q))

        @pl.when(up_terms)
        def _():
            wide_terms(dup, 1, t, q)
            down_terms(q)
            pl.when(q == CHIPS - 1)(lambda: put_d(t, lambda d: d.start()))


def backward(x, dy, weights, m, v):
    def dma(*shape):
        return pltpu.SemaphoreType.DMA(shape)

    def bf(*shape):
        return pltpu.VMEM(shape, BF)

    def f32(*shape):
        return pltpu.VMEM(shape, F32)

    message = (MR, LANE)
    outs = ((2, CHIPS, *message), message, (2, CHIPS, *message))
    anywhere = pl.BlockSpec(memory_space=pl.ANY)
    return pl.pallas_call(
        kernel,
        name="backward",
        out_shape=[jax.ShapeDtypeStruct((ROUNDS, *s), BF) for s in outs],
        in_specs=[anywhere] * 11,
        out_specs=[anywhere] * len(outs),
        scratch_shapes=[
            bf(KEPT, CHIPS, *message), bf(KEPT, CHIPS, *message), bf(CHIPS + 1, RING, *message), bf(3, SLOTS, *message), bf(SLOTS, *message), bf(SLOTS, *message),
            bf(*message), f32(*message), f32(*message), bf(SUB, D), f32(SUB, D), f32(SUB, D),
            bf(T, D), bf(T, D), bf(T, D), bf(D, T), bf(T, D), bf(D, T),
            bf(2, D, TILE), bf(2, D, TILE), bf(2, TILE, D),
            bf(T, TILE), bf(T, TILE), bf(T, TILE), f32(T, D), f32(T, D),
            bf(2, 2, CHIPS, *message), bf(CHIPS, 2, CHIPS, *message),
            dma(SLOTS), dma(KEPT), dma(3, SLOTS), dma(CHIPS + 1, RING), dma(KEPT), dma(3, 2), dma(5, SLOTS),
            dma(3, SLOTS), dma(CHIPS, RING), dma(3, SLOTS), dma(CHIPS, RING), dma(RING),
            dma(3), dma(3, 2), dma(2 + CHIPS),
        ],
        compiler_params=pltpu.CompilerParams(collective_id=0, has_side_effects=True, vmem_limit_bytes=67_043_328),
    )(x, dy, *weights, *m, *v)


DEPTH, STORES = 4, 3


def finish_kernel(*refs):
    def three(first):
        return refs[first : first + 3]

    news, grads, m, v = refs[0], refs[1], three(2), three(5)
    w_out, m_out, v_out = three(8), three(11), three(14)
    new_in, grad_in, m_in, v_in = three(17), three(20), three(23), three(26)
    w_to, m_to, v_to = three(29), three(32), three(35)
    sem_in, sem_out = refs[38:]
    steps = 2 * DEVICES

    def where(i):
        n, d = lax.div(i, DEVICES), lax.rem(i, DEVICES)
        wide, tall = pl.ds(pl.multiple_of(PIECE * d, PIECE), PIECE), pl.ds(pl.multiple_of(2 * SUB * d, 2 * SUB), 2 * SUB)
        return n, d, [(n, slice(None), wide)] * 2 + [(n, tall)]

    def loads(i, go):
        slot = lax.rem(i, DEPTH)
        n, d, states = where(i)
        core, chip, of = lax.rem(d, 2), lax.div(d, 2), 1 - n
        for kind in range(3):
            if kind < 2:
                grad = grads.at[of, :, kind, chip]
            else:
                grad = grads.at[of, chip, kind, pl.ds(2 * core, 2)]
            pairs = (
                (news.at[of, :, kind, :, core, chip], new_in[kind]),
                (grad, grad_in[kind]),
                (m[kind].at[states[kind]], m_in[kind]),
                (v[kind].at[states[kind]], v_in[kind]),
            )
            for number, (src, dst) in enumerate(pairs):
                go(pltpu.make_async_copy(src, dst.at[slot], sem_in.at[slot, kind, number]))

    def stores(i, go):
        slot = lax.rem(i, STORES)
        n, d, states = where(i)
        rows, tall = pl.ds(pl.multiple_of(ROWS * d, 16), ROWS), pl.ds(pl.multiple_of(TALL * d, TALL), TALL)
        for kind in range(3):
            pairs = (
                (w_to[kind], w_out[kind].at[n, rows if kind < 2 else tall]),
                (m_to[kind], m_out[kind].at[states[kind]]),
                (v_to[kind], v_out[kind].at[states[kind]]),
            )
            for number, (src, dst) in enumerate(pairs):
                go(pltpu.make_async_copy(src.at[slot], dst, sem_out.at[slot, kind, number]))

    for first in range(DEPTH):
        loads(first, lambda d: d.start())

    @times(steps)
    def _(i):
        slot, to, s = lax.rem(i, DEPTH), lax.rem(i, STORES), lax.rem(i, 2)
        loads(i, lambda d: d.wait())
        pl.when(i >= STORES)(lambda: stores(i - STORES, lambda d: d.wait()))

        def step(kind, rows, cols, g):
            old_m, old_v = m_in[kind][slot, rows, cols], v_in[kind][slot, rows, cols]
            m_to[kind][to, rows, cols], v_to[kind][to, rows, cols] = moments(old_m, old_v, g.astype(F32))

        for kind in range(2):
            for j in range(CHIPS):
                for q in range(CHIPS):
                    for half in range(2):
                        w_to[kind][to, :, cut(4 * (2 * q + half) + j, LANE)] = new_in[kind][slot, j, q, cut(half, ROWS)]
                step(kind, slice(ROWS), cut(j, LANE), grad_in[kind][slot, j, part(s, ROWS)])
        for number in range(D // LANE):
            for j in range(CHIPS):
                for q in range(CHIPS):
                    w_to[2][to, cut(CHIPS * j + q, SUB), cut(number, LANE)] = new_in[2][slot, j, q, cut(number, SUB)]
            for q in range(2):
                step(2, cut(q, SUB), cut(number, LANE), grad_in[2][slot, q, cut(number, SUB)])
        stores(i, lambda d: d.start())
        pl.when(i < steps - DEPTH)(lambda: loads(i + DEPTH, lambda d: d.start()))

    for last in range(STORES):
        stores(steps - STORES + last, lambda d: d.wait())


def finish(news, grads, m, v):
    shape = (2, CHIPS, 3, CHIPS)
    news, grads = news.reshape(*shape, 2, CHIPS, MR, LANE), grads.reshape(*shape, MR, LANE)
    anywhere = pl.BlockSpec(memory_space=pl.ANY)
    blocks = [(ROWS, PIECE), (ROWS, PIECE), (2 * SUB, D)]
    states = [jax.ShapeDtypeStruct(a.shape, F32) for a in m]
    return pl.pallas_call(
        finish_kernel,
        name="finish",
        out_shape=[*[jax.ShapeDtypeStruct((2, D, FF), BF)] * 2, jax.ShapeDtypeStruct((2, FF, D), BF), *states * 2],
        in_specs=[anywhere] * 8,
        out_specs=[anywhere] * 9,
        scratch_shapes=[
            *[pltpu.VMEM((DEPTH, CHIPS, CHIPS, MR, LANE), BF)] * 3,
            *[pltpu.VMEM((DEPTH, n, MR, LANE), BF) for n in (CHIPS, CHIPS, 2)],
            *[pltpu.VMEM((DEPTH, *b), F32) for b in blocks * 2],
            *[pltpu.VMEM((STORES, *b), BF) for b in ((ROWS, FF), (ROWS, FF), (TALL, D))],
            *[pltpu.VMEM((STORES, *b), F32) for b in blocks * 2],
            pltpu.SemaphoreType.DMA((DEPTH, 3, 4)), pltpu.SemaphoreType.DMA((STORES, 3, 3)),
        ],
        compiler_params=pltpu.CompilerParams(vmem_limit_bytes=60 * 2**20),
    )(news, grads, *m, *v)


def solution(mesh):
    def step(x, dy, *arrays):
        weights, m, v = (arrays[i : i + 3] for i in (0, 3, 6))
        news, grads, *_ = backward(x[0], dy[0], weights, m, v)
        return tuple(finish(news, grads, m, v))

    by_device, whole, rows = P(("rep", "dp")), P(), P(None, "dp")
    return jax.shard_map(
        step,
        mesh=mesh,
        in_specs=(by_device,) * 2 + (whole,) * 3 + (rows,) * 6,
        out_specs=(P("rep"),) * 3 + (P("rep", "dp"),) * 6,
        check_vma=False,
    )
```

```python
import jax
import jax.numpy as jnp
from jax import lax
from jax.experimental import pallas as pl
from jax.experimental.pallas import tpu as pltpu
from jax.sharding import PartitionSpec as P

MESH = pl.DeviceIdType.MESH
BF, F32 = jnp.bfloat16, jnp.float32

T, D, FF = 2048, 640, 4096
DEVICES, CHIPS, LANE = 8, 4, 128
TILE = DEVICES * LANE
ROWS, TALL = D // DEVICES, FF // DEVICES
PIECE, BLOCK = 512, 256
PARTS = 2

ROUNDS, MR, SUB = 96, 160, 32
PER_TILE = 12
D0, LAG, LAGF, LAGA, LAGD = 1, 2, 2, 2, 2
RING, SLOTS, KEPT = 16, 4, 12
TICKS = ROUNDS + D0 + 3 * LAG + LAGF + 2 * LAGA + max(LAGD, SLOTS)
AHEAD = 6


def normed(h):
    wide = h.astype(F32)
    scale = lax.rsqrt(jnp.mean(wide**2, -1, keepdims=True) + 1e-6)
    return (wide * scale).astype(BF)


def dot(a, b):
    return jnp.dot(a, b, preferred_element_type=F32)


def across(a, b):
    return lax.dot_general(a, b, (((1,), (1,)), ((), ())), preferred_element_type=F32)


def moments(m, v, g):
    return 0.9 * m + 0.1 * g, 0.95 * v + 0.05 * g * g


def within(r):
    return (r >= 0) & (r < ROUNDS)


def stage(n):
    t = lax.div(n, PER_TILE)
    return t, lax.rem(n, PER_TILE), lax.rem(t, CHIPS) == 0


def plan(r):
    t, i, early = stage(r + CHIPS)
    late = i - CHIPS
    kind = jnp.where(early, jnp.where(late < 0, 2, lax.rem(late, 2)), lax.rem(i, 3))
    q = jnp.where(early, jnp.where(late < 0, i, lax.div(late, 2)), lax.div(i, 3))
    t = t - lax.div(kind, 2)
    return PER_TILE * t + CHIPS * kind + q, t, kind, q


def ends_kind(r):
    _, i, early = stage(r + CHIPS)
    return jnp.where(early, (i == 3) | (i >= PER_TILE - 2), i >= PER_TILE - 3)


def most(zp):
    return jnp.maximum(zp, CHIPS - 1 - zp)


def part(i, n):
    return pl.ds(pl.multiple_of(n * i, n), n)


def cut(i, n):
    return slice(n * i, n * i + n)


def times(n, first=0):
    return pl.loop(first, n)


def kernel(
    x, dy, w_g, w_u, w_d, m_g, m_u, m_d, v_g, v_u, v_d,
    news, grads, terms,
    mine, others, line, summed, fresh, final, wb, mb, vb, wdb, mdb, vdb,
    hv, xv, av, at, ct, ctt, wgt, wut, wdt, act, dgate, dup, dag, dau, staged, staged_d,
    sem_pair_s, sem_pair_r, sem_line_s, sem_line_r, sem_mine, sem_state, sem_own, sem_ag_s, sem_ag_r, sem_agp_s, sem_agp_r, sem_own_r,
    sem_in, sem_w, sem_st,
):
    def tile(t):
        slot, of, j = lax.rem(t, 2), lax.rem(lax.div(t, CHIPS), 2), lax.rem(t, CHIPS)
        sems = [sem_w.at[i, slot] for i in range(3)]
        for d in range(DEVICES):
            cols, to = pl.ds(pl.multiple_of(TALL * d + LANE * j, LANE), LANE), pl.ds(LANE * d, LANE)
            pltpu.make_async_copy(w_g.at[of, :, cols], wgt.at[slot, :, to], sems[0]).start()
            pltpu.make_async_copy(w_u.at[of, :, cols], wut.at[slot, :, to], sems[1]).start()
            pltpu.make_async_copy(w_d.at[of, cols], wdt.at[slot, to], sems[2]).start()

    def plain_tile(t):
        slot, cols = lax.rem(t, 2), part(t, TILE)
        for i, (src, dst) in enumerate(((w_g.at[0, :, cols], wgt), (w_u.at[0, :, cols], wut), (w_d.at[0, cols], wdt))):
            pltpu.make_async_copy(src, dst.at[slot], sem_w.at[i, slot]).start()

    def tile_wait(t):
        slot, all_of = lax.rem(t, 2), pl.ds(0, TILE)
        sems = [sem_w.at[i, slot] for i in range(3)]
        pltpu.make_async_copy(w_g.at[0, :, all_of], wgt.at[slot], sems[0]).wait()
        pltpu.make_async_copy(w_u.at[0, :, all_of], wut.at[slot], sems[1]).wait()
        pltpu.make_async_copy(w_d.at[0, all_of], wdt.at[slot], sems[2]).wait()

    upper, lower = pl.ds(0, T // 2), pl.ds(T // 2, T // 2)
    load_x, load_more = (pltpu.make_async_copy(x.at[rows], xv.at[rows], sem_in.at[i]) for i, rows in enumerate((upper, lower)))
    load_dy = pltpu.make_async_copy(dy, ct, sem_in.at[2])
    load_x.start()
    plain_tile(0)
    load_more.start()
    load_dy.start()
    plain_tile(1)

    line[...] = jnp.zeros_like(line)
    me = lax.axis_index("dp")
    z, c = lax.div(me, 2), lax.rem(me, 2)
    partner = me + 1 - 2 * c
    low, high = z > 0, z < CHIPS - 1

    barrier = pltpu.get_barrier_semaphore()

    def greet(dev):
        pl.semaphore_signal(barrier, inc=1, device_id={"dp": dev}, device_id_type=MESH)

    greet(partner)
    pl.when(low)(lambda: greet(me - 2))
    pl.when(high)(lambda: greet(me + 2))

    def remote(src, dst, send, recv, dev):
        return pltpu.make_async_remote_copy(src, dst, send, recv, device_id={"dp": dev}, device_id_type=MESH)

    def pair(r, at_round=0):
        slot, kept = lax.rem(r, SLOTS), lax.rem(r, KEPT)
        return remote(terms.at[at_round, 1 - c], others.at[kept], sem_pair_s.at[slot], sem_pair_r.at[kept], partner)

    def own_terms(r, at_round=0):
        kept = lax.rem(r, KEPT)
        return pltpu.make_async_copy(terms.at[at_round, c], mine.at[kept], sem_mine.at[kept])

    def arrival(r, place):
        ring = lax.rem(r, RING)
        return remote(summed.at[0, 0], line.at[place, ring], sem_line_s.at[0, 0], sem_line_r.at[place, ring], partner)

    def on_chip(r, zp):
        kept = lax.rem(r, KEPT)
        return mine[kept, zp].astype(F32) + others[kept, zp].astype(F32)

    class Line:
        def __init__(self, i, k):
            self.i, self.zp = i, lax.rem(z + 1 + i, CHIPS)
            self.right = self.zp > z
            self.r = k - D0 - LAG * jnp.where(self.right, z, CHIPS - 1 - z)
            self.ok = within(self.r)
            self.fed = self.ok & jnp.where(self.right, low, high)

        def send(self, r):
            nxt = jnp.where(self.right, z + 1, z - 1)
            place = jnp.where((nxt == self.zp) & ~self.right, CHIPS, self.zp)
            slot, ring = lax.rem(r, SLOTS), lax.rem(r, RING)
            return remote(summed.at[self.i, slot], line.at[place, ring], sem_line_s.at[self.i, slot], sem_line_r.at[place, ring], 2 * nxt + c)

        def step(self):
            pl.when(within(self.r - SLOTS))(lambda: self.send(self.r - SLOTS).wait_send())
            pl.when(self.fed)(lambda: arrival(self.r, self.zp).wait_recv())

            @pl.when(self.ok)
            def _():
                total = on_chip(self.r, self.zp) + line[self.zp, lax.rem(self.r, RING)].astype(F32)
                summed[self.i, lax.rem(self.r, SLOTS)] = total.astype(BF)
                self.send(self.r).start()

    def state(r, go):
        _, t, kind, q = plan(r)
        of, j = 1 - lax.div(t, CHIPS), lax.rem(t, CHIPS)
        for number, (w, m, v) in enumerate(((w_g, m_g, v_g), (w_u, m_u, v_u))):

            @pl.when(kind == number)
            def _(w=w, m=m, v=v):
                rows = pl.ds(pl.multiple_of(ROWS * me, 16), ROWS)
                for s in range(2):
                    cols = pl.ds(pl.multiple_of(TALL * (2 * q + s) + LANE * j, LANE), LANE)
                    to, sems = pl.ds(ROWS * s, ROWS), [sem_state.at[i, s] for i in range(3)]
                    go(pltpu.make_async_copy(w.at[of, rows, cols], wb.at[to], sems[0]))
                    go(pltpu.make_async_copy(m.at[of, :, cols], mb.at[to], sems[1]))
                    go(pltpu.make_async_copy(v.at[of, :, cols], vb.at[to], sems[2]))

        @pl.when(kind == 2)
        def _():
            row, sems = pl.multiple_of(LANE * j + SUB * q, SUB), [sem_state.at[i, 0] for i in range(3)]
            rows = pl.ds(row, SUB)
            go(pltpu.make_async_copy(w_d.at[of, pl.ds(pl.multiple_of(TALL * me + row, SUB), SUB)], wdb, sems[0]))
            go(pltpu.make_async_copy(m_d.at[of, rows], mdb, sems[1]))
            go(pltpu.make_async_copy(v_d.at[of, rows], vdb, sems[2]))

    def adamw(w, m, v, g):
        m, v = moments(m, v, g.astype(F32))
        w = w.astype(F32)
        return (w - 0.02 * (m * lax.rsqrt(v + 1e-8) + 0.1 * w)).astype(BF)

    class Own:
        def __init__(self, k):
            self.r = k - D0 - LAG * most(z)
            self.ok = within(self.r)

        def outs(self, r, go, at_round=0):
            slot, ring = lax.rem(r, SLOTS), lax.rem(r, RING)
            src, dst = fresh.at[slot], news.at[at_round, c, z]
            pl.when(high)(lambda: go(remote(src, dst, sem_own.at[0, slot], sem_ag_r.at[z, ring], me + 2)))
            pl.when(low)(lambda: go(remote(src, dst, sem_own.at[1, slot], sem_ag_r.at[z, ring], me - 2)))
            go(remote(src, dst, sem_own.at[2, slot], sem_own_r.at[ring], partner))

        def local(self, r, go, at_round=0):
            slot = lax.rem(r, SLOTS)
            go(pltpu.make_async_copy(fresh.at[slot], news.at[at_round, c, z], sem_own.at[3, slot]))
            go(pltpu.make_async_copy(final.at[slot], grads.at[at_round], sem_own.at[4, slot]))

        def step(self):
            @pl.when(within(self.r - SLOTS))
            def _():
                self.outs(self.r - SLOTS, lambda d: d.wait_send())
                self.local(self.r - SLOTS, lambda d: d.wait())

            pl.when(self.ok & low)(lambda: arrival(self.r, z).wait_recv())
            pl.when(self.ok & high)(lambda: arrival(self.r, CHIPS).wait_recv())

            @pl.when(self.ok)
            def _():
                slot, ring = lax.rem(self.r, SLOTS), lax.rem(self.r, RING)
                at_round, _, kind, _ = plan(self.r)
                total = on_chip(self.r, z) + line[z, ring].astype(F32) + line[CHIPS, ring].astype(F32)
                final[slot] = total.astype(BF)
                state(self.r, lambda d: d.wait())

                @pl.when(kind == 2)
                def _():
                    for i in range(D // LANE):
                        rows, cols = pl.ds(SUB * i, SUB), pl.ds(LANE * i, LANE)
                        fresh[slot, rows] = adamw(wdb[:, cols], mdb[:, cols], vdb[:, cols], final[slot, rows])

                @pl.when(kind < 2)
                def _():
                    fresh[slot] = adamw(wb[...], mb[...], vb[...], final[slot])

                self.outs(self.r, lambda d: d.start(), at_round)
                self.local(self.r, lambda d: d.start(), at_round)

            pl.when(within(self.r + 1))(lambda: state(self.r + 1, lambda d: d.start()))

    def sent(k, zp):
        away = jnp.abs(z - zp)
        return k - D0 - LAG * most(zp) - LAGA * away - (LAGF - LAGA) * jnp.minimum(away, 1)

    class Gather:
        def __init__(self, i, k):
            self.i, self.zp = i, lax.rem(z + 1 + i, CHIPS)
            self.r, self.up = sent(k, self.zp), self.zp < z
            self.on = jnp.where(self.up, high, low)

        def forward(self, r, at_round=0):
            nxt, spot = jnp.where(self.up, z + 1, z - 1), news.at[at_round, c, self.zp]
            return remote(spot, spot, sem_ag_s.at[self.i, lax.rem(r, SLOTS)], sem_ag_r.at[self.zp, lax.rem(r, RING)], 2 * nxt + c)

        def over(self, r, at_round=CHIPS - 1):
            return bundle(r, at_round, c, self.zp, sem_agp_s.at[self.i, lax.rem(r, SLOTS)])

        def step(self):
            r, old, now = self.r, within(self.r - SLOTS), within(self.r)
            pl.when(old & self.on)(lambda: self.forward(r - SLOTS).wait_send())
            pl.when(old & ends_kind(r - SLOTS))(lambda: self.over(r - SLOTS).wait_send())

            @pl.when(now)
            def _():
                self.forward(r).wait_recv()
                at_round, _, _, q = plan(r)
                pl.when(self.on)(lambda: self.forward(r, at_round).start())
                pl.when(q == CHIPS - 1)(lambda: self.over(r, at_round).start())

    def bundle(r, at_round, core, zp, send):
        spot = news.at[pl.ds(at_round - (CHIPS - 1), CHIPS), core, zp]
        return remote(spot, spot, send, sem_agp_r.at[zp, lax.rem(r, RING)], partner)

    def tick(k):
        pl.when(within(k - SLOTS))(lambda: pair(k - SLOTS).wait_send())

        @pl.when(within(k - D0))
        def _():
            pair(k - D0).wait_recv()
            own_terms(k - D0).wait()

        for i in range(CHIPS - 1):
            Gather(i, k).step()
        for i in range(CHIPS - 1):
            Line(i, k).step()
        Own(k).step()
        r = sent(k, z) - LAGD
        spot = news.at[0, 1 - c, z]
        pl.when(within(r))(lambda: remote(spot, spot, sem_agp_s.at[0, 0], sem_own_r.at[lax.rem(r, RING)], partner).wait_recv())
        for i in range(CHIPS - 1):
            zp = lax.rem(z + 1 + i, CHIPS)
            r = sent(k, zp) - LAGD
            done = within(r) & ends_kind(r)
            pl.when(done)(lambda r=r, zp=zp: bundle(r, CHIPS - 1, 1 - c, zp, sem_agp_s.at[0, 0]).wait_recv())

    def begin_round(k):
        @pl.when(within(k))
        def _():
            at_round = plan(k)[0]
            pair(k, at_round).start()
            own_terms(k, at_round).start()

    half = T // 2
    blocks = half // BLOCK

    def enter(p):
        rows = part(p, BLOCK)
        av[rows] = normed(xv[rows])
        dag[rows] = jnp.zeros((BLOCK, D), F32)

    def hidden(t, p):
        slot, rows = lax.rem(t, 2), pl.ds(half * p, half)
        a = av[rows]
        for n in range(TILE // PIECE):
            cols = pl.ds(PIECE * n, PIECE)
            gate, up = dot(a, wgt[slot, :, cols]), dot(a, wut[slot, :, cols])
            act[rows, cols] = (gate * jax.nn.sigmoid(gate) * up).astype(BF)

    def turn(i):
        rows = part(i, BLOCK)
        ctt[:, rows] = ct[rows].T

    def back(t, p, n=half):
        rows = pl.ds(n * p, n)
        dag[rows] = dag[rows] + dot(act[rows], wdt[lax.rem(t, 2)])

    def leave(p):
        rows = part(p, BLOCK)
        h = xv[rows] + dag[rows].astype(BF)
        a = normed(h)
        hv[rows], av[rows], at[:, rows] = h, a, a.T
        dag[rows] = dau[rows] = jnp.zeros((BLOCK, D), F32)

    load_x.wait()
    times(blocks)(enter)
    tile_wait(0)
    load_more.wait()
    hidden(0, 0)
    for p in range(blocks):
        enter(blocks + p)
    load_dy.wait()
    turn(0)
    back(0, 0)
    hidden(0, 1)
    turn(1)

    @times(CHIPS, first=1)
    def _(t):
        tile_wait(t)
        back(t - 1, 1)
        hidden(t, 0)
        turn(2 * t)
        pl.when(t < CHIPS - 1)(lambda: plain_tile(t + 1))
        pl.when(t == CHIPS - 1)(lambda: tile(t + 1))
        back(t, 0)
        hidden(t, 1)
        turn(2 * t + 1)

    for third in range(2):
        back(CHIPS - 1, 2 + third, PIECE)
        for p in range(3):
            leave(3 * third + p)
    times(2 * blocks, first=2 * blocks - 2)(leave)

    def next_layer(q):
        @times(PIECE // BLOCK)
        def _(i):
            rows = part(PIECE // BLOCK * q + i, BLOCK)
            da = (dag[rows].astype(BF) + dau[rows].astype(BF)).astype(F32)
            wide = hv[rows].astype(F32)
            mean = jnp.mean(wide * wide, -1, keepdims=True) + 1e-6
            scale = lax.rsqrt(mean)
            along = jnp.sum(da * wide, -1, keepdims=True) * (-scale / (D * mean))
            by = ct[rows] + (da * scale + wide * along).astype(BF)
            a = normed(xv[rows])
            ct[rows], ctt[:, rows], av[rows], at[:, rows] = by, by.T, a, a.T

    def tokens(slot, q):
        cols = part(q, BLOCK)
        for p in range(PARTS):
            rows = pl.ds(T // PARTS * p, T // PARTS)
            a, by = av[rows], ct[rows]
            gate, up = dot(a, wgt[slot, :, cols]), dot(a, wut[slot, :, cols])
            dact = across(by, wdt[slot, cols]).astype(BF).astype(F32)
            sig = jax.nn.sigmoid(gate)
            silu = gate * sig
            act[rows, cols] = (silu * up).astype(BF)
            dup[rows, cols] = (dact * silu).astype(BF)
            dgate[rows, cols] = (dact * up * (sig + silu * (1.0 - sig))).astype(BF)

    def put(kind, r):
        return pltpu.make_async_copy(staged.at[kind], terms.at[r], sem_st.at[kind])

    def put_d(t, go):
        for q in range(CHIPS):
            go(pltpu.make_async_copy(staged_d.at[q], terms.at[PER_TILE * t + 2 * CHIPS + q], sem_st.at[2 + q]))

    def wide_terms(by, kind, q):
        g = dot(at[...], by[:, part(q, BLOCK)]).astype(BF)
        for d in range(DEVICES):
            for s in range(2):
                staged[kind, d % 2, d // 2, cut(s, ROWS)] = g[cut(d, ROWS), cut(s, LANE)]

    def puts(t, q):
        for kind in range(2):
            put(kind, PER_TILE * t + CHIPS * kind + q).start()

    def down_terms(i):
        g = dot(ctt[...], act[:, part(i, BLOCK)]).T.astype(BF)
        for o in range(2):
            for q in range(CHIPS):
                for s in range(D // LANE):
                    staged_d[q, o, i, cut(s, SUB)] = g[cut(CHIPS * o + q, SUB), cut(s, LANE)]

    sides = ((dag, dgate, wgt), (dau, dup, wut))

    def by_normed(which, slot, rows, side):
        (to, by, w), cols = sides[which], part(side, PIECE)
        to[rows] = to[rows] + across(by[rows, cols], w[slot, :, cols])

    pl.semaphore_wait(barrier, 1 + low.astype(jnp.int32) + high.astype(jnp.int32))

    def makes(n):
        _, i, early = stage(n)
        return (n >= CHIPS) & (n < ROUNDS) & jnp.where(early, (i > CHIPS) & (lax.rem(i, 2) == 1), lax.rem(i, 3) == 1)

    @times(TICKS + AHEAD, first=CHIPS)
    def _(n):
        t, i, early = stage(n)
        slot, busy = lax.rem(t, 2), n < ROUNDS
        q = jnp.where(early, lax.div(jnp.maximum(i - CHIPS, 0), 2), lax.div(i, 3))
        of_three = lax.rem(i, 3)
        starts = jnp.where(early, (i >= CHIPS) & (lax.rem(i, 2) == 0), of_three == 0)

        @pl.when(busy & starts & (q == 0))
        def _():
            tile_wait(t)

        pl.when((i == CHIPS + 2) & (n < ROUNDS - PER_TILE))(lambda: tile(t + CHIPS + 1))

        tick(n - AHEAD)

        @pl.when(makes(n - 1))
        def _():
            put(0, 0).wait()
            put(1, 0).wait()

        pl.when((i == 1) & (n >= PER_TILE) & (n < ROUNDS + PER_TILE))(lambda: put_d(0, lambda d: d.wait()))
        begin_round(n - AHEAD)

        ends = busy & ~early & (of_three == 2)
        inner, turning = t < CHIPS, (t == CHIPS) & (i < CHIPS)
        before = q < 2
        share = (jnp.where(before, 1 - slot, slot), part(lax.rem(q, 2), half), before.astype(jnp.int32))
        own_share = (slot, part(lax.div(i - 2 * CHIPS, 2), half), 0)
        late = (t == 0) & (i >= 2 * CHIPS)

        @pl.when(turning)
        def _():
            for which in range(2):
                by_normed(which, 1 - slot, part(i, PIECE), 1)
            next_layer(i)

        pl.when(busy & starts)(lambda: tokens(slot, q))

        @pl.when(makes(n) & early)
        def _():
            wide_terms(dgate, 0, q)
            wide_terms(dup, 1, q)
            down_terms(q)
            puts(t, q)

        for which in range(2):
            pl.when(late & (lax.rem(i, 2) == which))(lambda which=which: by_normed(which, *own_share))

        @pl.when(makes(n) & ~early & inner)
        def _():
            wide_terms(dgate, 0, q)
            wide_terms(dup, 1, q)
            by_normed(0, *share)
            puts(t, q)

        @pl.when(makes(n) & ~early & ~inner)
        def _():
            wide_terms(dgate, 0, q)
            wide_terms(dup, 1, q)
            puts(t, q)

        @pl.when(ends & inner)
        def _():
            down_terms(q)
            by_normed(1, *share)

        pl.when(ends & ~inner)(lambda: down_terms(q))
        pl.when(busy & (i == PER_TILE - 1))(lambda: put_d(t, lambda d: d.start()))


def backward(x, dy, weights, m, v):
    def dma(*shape):
        return pltpu.SemaphoreType.DMA(shape)

    def bf(*shape):
        return pltpu.VMEM(shape, BF)

    def f32(*shape):
        return pltpu.VMEM(shape, F32)

    message = (MR, LANE)
    outs = ((2, CHIPS, *message), message, (2, CHIPS, *message))
    anywhere = pl.BlockSpec(memory_space=pl.ANY)
    return pl.pallas_call(
        kernel,
        name="backward",
        out_shape=[jax.ShapeDtypeStruct((ROUNDS, *s), BF) for s in outs],
        in_specs=[anywhere] * 11,
        out_specs=[anywhere] * len(outs),
        scratch_shapes=[
            bf(KEPT, CHIPS, *message), bf(KEPT, CHIPS, *message), bf(CHIPS + 1, RING, *message), bf(3, SLOTS, *message), bf(SLOTS, *message), bf(SLOTS, *message),
            bf(*message), f32(*message), f32(*message), bf(SUB, D), f32(SUB, D), f32(SUB, D),
            bf(T, D), bf(T, D), bf(T, D), bf(D, T), bf(T, D), bf(D, T),
            bf(2, D, TILE), bf(2, D, TILE), bf(2, TILE, D),
            bf(T, TILE), bf(T, TILE), bf(T, TILE), f32(T, D), f32(T, D),
            bf(2, 2, CHIPS, *message), bf(CHIPS, 2, CHIPS, *message),
            dma(SLOTS), dma(KEPT), dma(3, SLOTS), dma(CHIPS + 1, RING), dma(KEPT), dma(3, 2), dma(5, SLOTS),
            dma(3, SLOTS), dma(CHIPS, RING), dma(3, SLOTS), dma(CHIPS, RING), dma(RING),
            dma(3), dma(3, 2), dma(2 + CHIPS),
        ],
        compiler_params=pltpu.CompilerParams(collective_id=0, has_side_effects=True, vmem_limit_bytes=67_043_328),
    )(x, dy, *weights, *m, *v)


DEPTH, STORES = 4, 3


def finish_kernel(*refs):
    def three(first):
        return refs[first : first + 3]

    news, grads, m, v = refs[0], refs[1], three(2), three(5)
    w_out, m_out, v_out = three(8), three(11), three(14)
    new_in, grad_in, m_in, v_in = three(17), three(20), three(23), three(26)
    w_to, m_to, v_to = three(29), three(32), three(35)
    sem_in, sem_out = refs[38:]
    steps = 2 * DEVICES

    def where(i):
        n, d = lax.div(i, DEVICES), lax.rem(i, DEVICES)
        wide, tall = pl.ds(pl.multiple_of(PIECE * d, PIECE), PIECE), pl.ds(pl.multiple_of(2 * SUB * d, 2 * SUB), 2 * SUB)
        return n, d, [(n, slice(None), wide)] * 2 + [(n, tall)]

    def loads(i, go):
        slot = lax.rem(i, DEPTH)
        n, d, states = where(i)
        core, chip, of = lax.rem(d, 2), lax.div(d, 2), 1 - n
        for kind in range(3):
            if kind < 2:
                grad = grads.at[of, :, kind, chip, part(core, ROWS)]
            else:
                grad = grads.at[of, chip, kind, pl.ds(2 * core, 2)]
            pairs = (
                (news.at[of, :, kind, :, core, chip], new_in[kind]),
                (grad, grad_in[kind]),
                (m[kind].at[states[kind]], m_in[kind]),
                (v[kind].at[states[kind]], v_in[kind]),
            )
            for number, (src, dst) in enumerate(pairs):
                go(pltpu.make_async_copy(src, dst.at[slot], sem_in.at[slot, kind, number]))

    def stores(i, go):
        slot = lax.rem(i, STORES)
        n, d, states = where(i)
        rows, tall = pl.ds(pl.multiple_of(ROWS * d, 16), ROWS), pl.ds(pl.multiple_of(TALL * d, TALL), TALL)
        for kind in range(3):
            pairs = (
                (w_to[kind], w_out[kind].at[n, rows if kind < 2 else tall]),
                (m_to[kind], m_out[kind].at[states[kind]]),
                (v_to[kind], v_out[kind].at[states[kind]]),
            )
            for number, (src, dst) in enumerate(pairs):
                go(pltpu.make_async_copy(src.at[slot], dst, sem_out.at[slot, kind, number]))

    for first in range(DEPTH):
        loads(first, lambda d: d.start())

    @times(steps)
    def _(i):
        slot, to = lax.rem(i, DEPTH), lax.rem(i, STORES)
        loads(i, lambda d: d.wait())
        pl.when(i >= STORES)(lambda: stores(i - STORES, lambda d: d.wait()))

        def step(kind, rows, cols, g):
            old_m, old_v = m_in[kind][slot, rows, cols], v_in[kind][slot, rows, cols]
            m_to[kind][to, rows, cols], v_to[kind][to, rows, cols] = moments(old_m, old_v, g.astype(F32))

        for kind in range(2):
            for j in range(CHIPS):
                for q in range(CHIPS):
                    for half in range(2):
                        w_to[kind][to, :, cut(4 * (2 * q + half) + j, LANE)] = new_in[kind][slot, j, q, cut(half, ROWS)]
                step(kind, slice(ROWS), cut(j, LANE), grad_in[kind][slot, j])
        for number in range(D // LANE):
            for j in range(CHIPS):
                for q in range(CHIPS):
                    w_to[2][to, cut(CHIPS * j + q, SUB), cut(number, LANE)] = new_in[2][slot, j, q, cut(number, SUB)]
            for q in range(2):
                step(2, cut(q, SUB), cut(number, LANE), grad_in[2][slot, q, cut(number, SUB)])
        stores(i, lambda d: d.start())
        pl.when(i < steps - DEPTH)(lambda: loads(i + DEPTH, lambda d: d.start()))

    for last in range(STORES):
        stores(steps - STORES + last, lambda d: d.wait())


def finish(news, grads, m, v):
    shape = (2, CHIPS, 3, CHIPS)
    news, grads = news.reshape(*shape, 2, CHIPS, MR, LANE), grads.reshape(*shape, MR, LANE)
    anywhere = pl.BlockSpec(memory_space=pl.ANY)
    blocks = [(ROWS, PIECE), (ROWS, PIECE), (2 * SUB, D)]
    states = [jax.ShapeDtypeStruct(a.shape, F32) for a in m]
    return pl.pallas_call(
        finish_kernel,
        name="finish",
        out_shape=[*[jax.ShapeDtypeStruct((2, D, FF), BF)] * 2, jax.ShapeDtypeStruct((2, FF, D), BF), *states * 2],
        in_specs=[anywhere] * 8,
        out_specs=[anywhere] * 9,
        scratch_shapes=[
            *[pltpu.VMEM((DEPTH, CHIPS, CHIPS, MR, LANE), BF)] * 3,
            *[pltpu.VMEM((DEPTH, *b, LANE), BF) for b in ((CHIPS, ROWS), (CHIPS, ROWS), (2, MR))],
            *[pltpu.VMEM((DEPTH, *b), F32) for b in blocks * 2],
            *[pltpu.VMEM((STORES, *b), BF) for b in ((ROWS, FF), (ROWS, FF), (TALL, D))],
            *[pltpu.VMEM((STORES, *b), F32) for b in blocks * 2],
            pltpu.SemaphoreType.DMA((DEPTH, 3, 4)), pltpu.SemaphoreType.DMA((STORES, 3, 3)),
        ],
        compiler_params=pltpu.CompilerParams(vmem_limit_bytes=60 * 2**20),
    )(news, grads, *m, *v)


def solution(mesh):
    def step(x, dy, *arrays):
        weights, m, v = (arrays[i : i + 3] for i in (0, 3, 6))
        news, grads, *_ = backward(x[0], dy[0], weights, m, v)
        return tuple(finish(news, grads, m, v))

    by_device, whole, rows = P(("rep", "dp")), P(), P(None, "dp")
    return jax.shard_map(
        step,
        mesh=mesh,
        in_specs=(by_device,) * 2 + (whole,) * 3 + (rows,) * 6,
        out_specs=(P("rep"),) * 3 + (P("rep", "dp"),) * 6,
        check_vma=False,
    )
```

```python
import jax
import jax.numpy as jnp
from jax import lax
from jax.experimental import pallas as pl
from jax.experimental.pallas import tpu as pltpu
from jax.sharding import PartitionSpec as P

MESH = pl.DeviceIdType.MESH
BF, F32 = jnp.bfloat16, jnp.float32

T, D, FF = 2048, 640, 4096
DEVICES, CHIPS, LANE = 8, 4, 128
TILE = DEVICES * LANE
ROWS, TALL = D // DEVICES, FF // DEVICES
PIECE, BLOCK = 512, 256
PARTS = 2
KEEP = 2 * 3 * T * TILE + 2 * 2 * D * T + 4 * T * D

ROUNDS, MR, SUB = 96, 160, 32
PER_TILE = 12
D0, LAG, LAGF, LAGA, LAGD = 1, 2, 2, 2, 2
RING, SLOTS, KEPT = 16, 4, 12
TICKS = ROUNDS + D0 + 3 * LAG + LAGF + 2 * LAGA + max(LAGD, SLOTS)
AHEAD = 6


def normed(h):
    wide = h.astype(F32)
    scale = lax.rsqrt(jnp.mean(wide**2, -1, keepdims=True) + 1e-6)
    return (wide * scale).astype(BF)


def dot(a, b):
    return jnp.dot(a, b, preferred_element_type=F32)


def across(a, b):
    return lax.dot_general(a, b, (((1,), (1,)), ((), ())), preferred_element_type=F32)


def moments(m, v, g):
    return 0.9 * m + 0.1 * g, 0.95 * v + 0.05 * g * g


def within(r):
    return (r >= 0) & (r < ROUNDS)


def stage(n):
    t = lax.div(n, PER_TILE)
    return t, lax.rem(n, PER_TILE), lax.rem(t, CHIPS) == 0


def plan(r):
    t, i, early = stage(r + CHIPS)
    late = i - CHIPS
    kind = jnp.where(early, jnp.where(late < 0, 2, lax.rem(late, 2)), lax.rem(i, 3))
    q = jnp.where(early, jnp.where(late < 0, i, lax.div(late, 2)), lax.div(i, 3))
    t = t - lax.div(kind, 2)
    return PER_TILE * t + CHIPS * kind + q, t, kind, q


def ends_kind(r):
    _, i, early = stage(r + CHIPS)
    return jnp.where(early, (i == 3) | (i >= PER_TILE - 2), i >= PER_TILE - 3)


def most(zp):
    return jnp.maximum(zp, CHIPS - 1 - zp)


def part(i, n):
    return pl.ds(pl.multiple_of(n * i, n), n)


def cut(i, n):
    return slice(n * i, n * i + n)


def times(n, first=0):
    return pl.loop(first, n)


def kernel(
    x, dy, w_g, w_u, w_d, m_g, m_u, m_d, v_g, v_u, v_d,
    news, grads, terms, act, dgate, dup, dag, at, ctt,
    mine, others, line, summed, fresh, final, wb, mb, vb, wdb, mdb, vdb,
    hv, xv, av, ct, wgt, wut, wdt, dau, staged, staged_d,
    sem_pair_s, sem_pair_r, sem_line_s, sem_line_r, sem_mine, sem_state, sem_own, sem_ag_s, sem_ag_r, sem_agp_s, sem_agp_r, sem_own_r,
    sem_in, sem_w, sem_st, sem_keep,
):
    def tile(t):
        slot, of, j = lax.rem(t, 2), lax.rem(lax.div(t, CHIPS), 2), lax.rem(t, CHIPS)
        sems = [sem_w.at[i, slot] for i in range(3)]
        for d in range(DEVICES):
            cols, to = pl.ds(pl.multiple_of(TALL * d + LANE * j, LANE), LANE), pl.ds(LANE * d, LANE)
            pltpu.make_async_copy(w_g.at[of, :, cols], wgt.at[slot, :, to], sems[0]).start()
            pltpu.make_async_copy(w_u.at[of, :, cols], wut.at[slot, :, to], sems[1]).start()
            pltpu.make_async_copy(w_d.at[of, cols], wdt.at[slot, to], sems[2]).start()

    def plain_tile(t):
        slot, cols = lax.rem(t, 2), part(t, TILE)
        for i, (src, dst) in enumerate(((w_g.at[0, :, cols], wgt), (w_u.at[0, :, cols], wut), (w_d.at[0, cols], wdt))):
            pltpu.make_async_copy(src, dst.at[slot], sem_w.at[i, slot]).start()

    def tile_wait(t):
        slot, all_of = lax.rem(t, 2), pl.ds(0, TILE)
        sems = [sem_w.at[i, slot] for i in range(3)]
        pltpu.make_async_copy(w_g.at[0, :, all_of], wgt.at[slot], sems[0]).wait()
        pltpu.make_async_copy(w_u.at[0, :, all_of], wut.at[slot], sems[1]).wait()
        pltpu.make_async_copy(w_d.at[0, all_of], wdt.at[slot], sems[2]).wait()

    upper, lower = pl.ds(0, T // 2), pl.ds(T // 2, T // 2)
    load_x, load_more = (pltpu.make_async_copy(x.at[rows], xv.at[rows], sem_in.at[i]) for i, rows in enumerate((upper, lower)))
    load_dy = pltpu.make_async_copy(dy, ct, sem_in.at[2])
    load_x.start()
    plain_tile(0)
    load_more.start()
    load_dy.start()
    plain_tile(1)

    line[...] = jnp.zeros_like(line)
    me = lax.axis_index("dp")
    z, c = lax.div(me, 2), lax.rem(me, 2)
    partner = me + 1 - 2 * c
    low, high = z > 0, z < CHIPS - 1

    barrier = pltpu.get_barrier_semaphore()

    def greet(dev):
        pl.semaphore_signal(barrier, inc=1, device_id={"dp": dev}, device_id_type=MESH)

    greet(partner)
    pl.when(low)(lambda: greet(me - 2))
    pl.when(high)(lambda: greet(me + 2))

    def remote(src, dst, send, recv, dev):
        return pltpu.make_async_remote_copy(src, dst, send, recv, device_id={"dp": dev}, device_id_type=MESH)

    def pair(r, at_round=0):
        slot, kept = lax.rem(r, SLOTS), lax.rem(r, KEPT)
        return remote(terms.at[at_round, 1 - c], others.at[kept], sem_pair_s.at[slot], sem_pair_r.at[kept], partner)

    def own_terms(r, at_round=0):
        kept = lax.rem(r, KEPT)
        return pltpu.make_async_copy(terms.at[at_round, c], mine.at[kept], sem_mine.at[kept])

    def arrival(r, place):
        ring = lax.rem(r, RING)
        return remote(summed.at[0, 0], line.at[place, ring], sem_line_s.at[0, 0], sem_line_r.at[place, ring], partner)

    def on_chip(r, zp):
        kept = lax.rem(r, KEPT)
        return mine[kept, zp].astype(F32) + others[kept, zp].astype(F32)

    class Line:
        def __init__(self, i, k):
            self.i, self.zp = i, lax.rem(z + 1 + i, CHIPS)
            self.right = self.zp > z
            self.r = k - D0 - LAG * jnp.where(self.right, z, CHIPS - 1 - z)
            self.ok = within(self.r)
            self.fed = self.ok & jnp.where(self.right, low, high)

        def send(self, r):
            nxt = jnp.where(self.right, z + 1, z - 1)
            place = jnp.where((nxt == self.zp) & ~self.right, CHIPS, self.zp)
            slot, ring = lax.rem(r, SLOTS), lax.rem(r, RING)
            return remote(summed.at[self.i, slot], line.at[place, ring], sem_line_s.at[self.i, slot], sem_line_r.at[place, ring], 2 * nxt + c)

        def step(self):
            pl.when(within(self.r - SLOTS))(lambda: self.send(self.r - SLOTS).wait_send())
            pl.when(self.fed)(lambda: arrival(self.r, self.zp).wait_recv())

            @pl.when(self.ok)
            def _():
                total = on_chip(self.r, self.zp) + line[self.zp, lax.rem(self.r, RING)].astype(F32)
                summed[self.i, lax.rem(self.r, SLOTS)] = total.astype(BF)
                self.send(self.r).start()

    def state(r, go):
        _, t, kind, q = plan(r)
        of, j = 1 - lax.div(t, CHIPS), lax.rem(t, CHIPS)
        for number, (w, m, v) in enumerate(((w_g, m_g, v_g), (w_u, m_u, v_u))):

            @pl.when(kind == number)
            def _(w=w, m=m, v=v):
                rows = pl.ds(pl.multiple_of(ROWS * me, 16), ROWS)
                for s in range(2):
                    cols = pl.ds(pl.multiple_of(TALL * (2 * q + s) + LANE * j, LANE), LANE)
                    to, sems = pl.ds(ROWS * s, ROWS), [sem_state.at[i, s] for i in range(3)]
                    go(pltpu.make_async_copy(w.at[of, rows, cols], wb.at[to], sems[0]))
                    go(pltpu.make_async_copy(m.at[of, :, cols], mb.at[to], sems[1]))
                    go(pltpu.make_async_copy(v.at[of, :, cols], vb.at[to], sems[2]))

        @pl.when(kind == 2)
        def _():
            row, sems = pl.multiple_of(LANE * j + SUB * q, SUB), [sem_state.at[i, 0] for i in range(3)]
            rows = pl.ds(row, SUB)
            go(pltpu.make_async_copy(w_d.at[of, pl.ds(pl.multiple_of(TALL * me + row, SUB), SUB)], wdb, sems[0]))
            go(pltpu.make_async_copy(m_d.at[of, rows], mdb, sems[1]))
            go(pltpu.make_async_copy(v_d.at[of, rows], vdb, sems[2]))

    def adamw(w, m, v, g):
        m, v = moments(m, v, g.astype(F32))
        w = w.astype(F32)
        return (w - 0.02 * (m * lax.rsqrt(v + 1e-8) + 0.1 * w)).astype(BF)

    class Own:
        def __init__(self, k):
            self.r = k - D0 - LAG * most(z)
            self.ok = within(self.r)

        def outs(self, r, go, at_round=0):
            slot, ring = lax.rem(r, SLOTS), lax.rem(r, RING)
            src, dst = fresh.at[slot], news.at[at_round, c, z]
            pl.when(high)(lambda: go(remote(src, dst, sem_own.at[0, slot], sem_ag_r.at[z, ring], me + 2)))
            pl.when(low)(lambda: go(remote(src, dst, sem_own.at[1, slot], sem_ag_r.at[z, ring], me - 2)))
            go(remote(src, dst, sem_own.at[2, slot], sem_own_r.at[ring], partner))

        def local(self, r, go, at_round=0):
            slot = lax.rem(r, SLOTS)
            go(pltpu.make_async_copy(fresh.at[slot], news.at[at_round, c, z], sem_own.at[3, slot]))
            go(pltpu.make_async_copy(final.at[slot], grads.at[at_round], sem_own.at[4, slot]))

        def step(self):
            @pl.when(within(self.r - SLOTS))
            def _():
                self.outs(self.r - SLOTS, lambda d: d.wait_send())
                self.local(self.r - SLOTS, lambda d: d.wait())

            pl.when(self.ok & low)(lambda: arrival(self.r, z).wait_recv())
            pl.when(self.ok & high)(lambda: arrival(self.r, CHIPS).wait_recv())

            @pl.when(self.ok)
            def _():
                slot, ring = lax.rem(self.r, SLOTS), lax.rem(self.r, RING)
                at_round, _, kind, _ = plan(self.r)
                total = on_chip(self.r, z) + line[z, ring].astype(F32) + line[CHIPS, ring].astype(F32)
                final[slot] = total.astype(BF)
                state(self.r, lambda d: d.wait())

                @pl.when(kind == 2)
                def _():
                    for i in range(D // LANE):
                        rows, cols = pl.ds(SUB * i, SUB), pl.ds(LANE * i, LANE)
                        fresh[slot, rows] = adamw(wdb[:, cols], mdb[:, cols], vdb[:, cols], final[slot, rows])

                @pl.when(kind < 2)
                def _():
                    fresh[slot] = adamw(wb[...], mb[...], vb[...], final[slot])

                self.outs(self.r, lambda d: d.start(), at_round)
                self.local(self.r, lambda d: d.start(), at_round)

            pl.when(within(self.r + 1))(lambda: state(self.r + 1, lambda d: d.start()))

    def sent(k, zp):
        away = jnp.abs(z - zp)
        return k - D0 - LAG * most(zp) - LAGA * away - (LAGF - LAGA) * jnp.minimum(away, 1)

    class Gather:
        def __init__(self, i, k):
            self.i, self.zp = i, lax.rem(z + 1 + i, CHIPS)
            self.r, self.up = sent(k, self.zp), self.zp < z
            self.on = jnp.where(self.up, high, low)

        def forward(self, r, at_round=0):
            nxt, spot = jnp.where(self.up, z + 1, z - 1), news.at[at_round, c, self.zp]
            return remote(spot, spot, sem_ag_s.at[self.i, lax.rem(r, SLOTS)], sem_ag_r.at[self.zp, lax.rem(r, RING)], 2 * nxt + c)

        def over(self, r, at_round=CHIPS - 1):
            return bundle(r, at_round, c, self.zp, sem_agp_s.at[self.i, lax.rem(r, SLOTS)])

        def step(self):
            r, old, now = self.r, within(self.r - SLOTS), within(self.r)
            pl.when(old & self.on)(lambda: self.forward(r - SLOTS).wait_send())
            pl.when(old & ends_kind(r - SLOTS))(lambda: self.over(r - SLOTS).wait_send())

            @pl.when(now)
            def _():
                self.forward(r).wait_recv()
                at_round, _, _, q = plan(r)
                pl.when(self.on)(lambda: self.forward(r, at_round).start())
                pl.when(q == CHIPS - 1)(lambda: self.over(r, at_round).start())

    def bundle(r, at_round, core, zp, send):
        spot = news.at[pl.ds(at_round - (CHIPS - 1), CHIPS), core, zp]
        return remote(spot, spot, send, sem_agp_r.at[zp, lax.rem(r, RING)], partner)

    def tick(k):
        pl.when(within(k - SLOTS))(lambda: pair(k - SLOTS).wait_send())

        @pl.when(within(k - D0))
        def _():
            pair(k - D0).wait_recv()
            own_terms(k - D0).wait()

        for i in range(CHIPS - 1):
            Gather(i, k).step()
        for i in range(CHIPS - 1):
            Line(i, k).step()
        Own(k).step()
        r = sent(k, z) - LAGD
        spot = news.at[0, 1 - c, z]
        pl.when(within(r))(lambda: remote(spot, spot, sem_agp_s.at[0, 0], sem_own_r.at[lax.rem(r, RING)], partner).wait_recv())
        for i in range(CHIPS - 1):
            zp = lax.rem(z + 1 + i, CHIPS)
            r = sent(k, zp) - LAGD
            done = within(r) & ends_kind(r)
            pl.when(done)(lambda r=r, zp=zp: bundle(r, CHIPS - 1, 1 - c, zp, sem_agp_s.at[0, 0]).wait_recv())

    def begin_round(k):
        @pl.when(within(k))
        def _():
            at_round = plan(k)[0]
            pair(k, at_round).start()
            own_terms(k, at_round).start()

    half = T // 2
    blocks = half // BLOCK

    def enter(p):
        rows = part(p, BLOCK)
        av[rows] = normed(xv[rows])
        dag[rows] = jnp.zeros((BLOCK, D), F32)

    def hidden(t, p):
        slot, rows = lax.rem(t, 2), pl.ds(half * p, half)
        a = av[rows]
        for n in range(TILE // PIECE):
            cols = pl.ds(PIECE * n, PIECE)
            gate, up = dot(a, wgt[slot, :, cols]), dot(a, wut[slot, :, cols])
            act[rows, cols] = (gate * jax.nn.sigmoid(gate) * up).astype(BF)

    def turn(i):
        rows = part(i, BLOCK)
        ctt[:, rows] = ct[rows].T

    def back(t, p, n=half):
        rows = pl.ds(n * p, n)
        dag[rows] = dag[rows] + dot(act[rows], wdt[lax.rem(t, 2)])

    def leave(p):
        rows = part(p, BLOCK)
        h = xv[rows] + dag[rows].astype(BF)
        a = normed(h)
        hv[rows], av[rows], at[:, rows] = h, a, a.T
        dag[rows] = dau[rows] = jnp.zeros((BLOCK, D), F32)

    load_x.wait()
    times(blocks)(enter)
    tile_wait(0)
    load_more.wait()
    hidden(0, 0)
    for p in range(blocks):
        enter(blocks + p)
    load_dy.wait()
    turn(0)
    back(0, 0)
    hidden(0, 1)
    turn(1)

    @times(CHIPS, first=1)
    def _(t):
        tile_wait(t)
        back(t - 1, 1)
        hidden(t, 0)
        turn(2 * t)
        pl.when(t < CHIPS - 1)(lambda: plain_tile(t + 1))
        pl.when(t == CHIPS - 1)(lambda: tile(t + 1))
        back(t, 0)
        hidden(t, 1)
        turn(2 * t + 1)

    for third in range(2):
        back(CHIPS - 1, 2 + third, PIECE)
        for p in range(3):
            leave(3 * third + p)
    times(2 * blocks, first=2 * blocks - 2)(leave)

    def next_layer(q):
        @times(PIECE // BLOCK)
        def _(i):
            rows = part(PIECE // BLOCK * q + i, BLOCK)
            da = (dag[rows].astype(BF) + dau[rows].astype(BF)).astype(F32)
            wide = hv[rows].astype(F32)
            mean = jnp.mean(wide * wide, -1, keepdims=True) + 1e-6
            scale = lax.rsqrt(mean)
            along = jnp.sum(da * wide, -1, keepdims=True) * (-scale / (D * mean))
            by = ct[rows] + (da * scale + wide * along).astype(BF)
            a = normed(xv[rows])
            ct[rows], ctt[:, rows], av[rows], at[:, rows] = by, by.T, a, a.T

    def tokens(slot, q):
        cols = part(q, BLOCK)
        for p in range(PARTS):
            rows = pl.ds(T // PARTS * p, T // PARTS)
            a, by = av[rows], ct[rows]
            gate, up = dot(a, wgt[slot, :, cols]), dot(a, wut[slot, :, cols])
            dact = across(by, wdt[slot, cols]).astype(BF).astype(F32)
            sig = jax.nn.sigmoid(gate)
            silu = gate * sig
            act[rows, cols] = (silu * up).astype(BF)
            dup[rows, cols] = (dact * silu).astype(BF)
            dgate[rows, cols] = (dact * up * (sig + silu * (1.0 - sig))).astype(BF)

    def put(kind, r):
        return pltpu.make_async_copy(staged.at[kind], terms.at[r], sem_st.at[kind])

    def put_d(t, go):
        for q in range(CHIPS):
            go(pltpu.make_async_copy(staged_d.at[q], terms.at[PER_TILE * t + 2 * CHIPS + q], sem_st.at[2 + q]))

    def wide_terms(by, kind, q):
        g = dot(at[...], by[:, part(q, BLOCK)]).astype(BF)
        for d in range(DEVICES):
            for s in range(2):
                staged[kind, d % 2, d // 2, cut(s, ROWS)] = g[cut(d, ROWS), cut(s, LANE)]

    def puts(t, q):
        for kind in range(2):
            put(kind, PER_TILE * t + CHIPS * kind + q).start()

    def down_terms(i):
        g = dot(ctt[...], act[:, part(i, BLOCK)]).T.astype(BF)
        for o in range(2):
            for q in range(CHIPS):
                for s in range(D // LANE):
                    staged_d[q, o, i, cut(s, SUB)] = g[cut(CHIPS * o + q, SUB), cut(s, LANE)]

    sides = ((dag, dgate, wgt), (dau, dup, wut))

    def by_normed(which, slot, rows, side):
        (to, by, w), cols = sides[which], part(side, PIECE)
        to[rows] = to[rows] + across(by[rows, cols], w[slot, :, cols])

    pl.semaphore_wait(barrier, 1 + low.astype(jnp.int32) + high.astype(jnp.int32))

    def states_kept(go):
        for i, src in enumerate((m_d, v_d)):
            for of in range(2):
                place = 2 * i + of
                go(pltpu.make_async_copy(src.at[of], dag.at[cut(place, TALL)], sem_keep.at[5 + place]))

    def keep(e):
        d, kind = lax.div(e, 2), lax.rem(e, 2)
        core, chip = lax.rem(d, 2), lax.div(d, 2)
        pl.when(e == 0)(lambda: states_kept(lambda c: c.start()))

        def take(j, q, kind, buf, row, col, number):
            to = buf.at[pl.ds(pl.multiple_of(MR * row, MR), MR), cut(col, LANE)]
            pltpu.make_async_copy(news.at[PER_TILE * j + CHIPS * kind + q, core, chip], to, sem_keep.at[number]).start()

        for number, buf in enumerate((act, dgate, dup)):

            @pl.when(lax.div(d, 3) == number)
            def _(number=number, buf=buf):
                for j in range(CHIPS):
                    for q in range(CHIPS):
                        take(j, q, kind, buf, CHIPS * lax.rem(d, 3) + 2 * kind + j // 2, CHIPS * (j % 2) + q, number)

        for number, buf in enumerate((at, ctt)):

            @pl.when((kind == 0) & (lax.div(d, CHIPS) == number))
            def _(number=number, buf=buf):
                for j in range(CHIPS):
                    for q in range(CHIPS):
                        take(j, q, 2, buf, lax.rem(d, CHIPS), CHIPS * j + q, 3 + number)

    def makes(n):
        _, i, early = stage(n)
        return (n >= CHIPS) & (n < ROUNDS) & jnp.where(early, (i > CHIPS) & (lax.rem(i, 2) == 1), lax.rem(i, 3) == 1)

    @times(TICKS + AHEAD, first=CHIPS)
    def _(n):
        t, i, early = stage(n)
        slot, busy = lax.rem(t, 2), n < ROUNDS
        q = jnp.where(early, lax.div(jnp.maximum(i - CHIPS, 0), 2), lax.div(i, 3))
        of_three = lax.rem(i, 3)
        starts = jnp.where(early, (i >= CHIPS) & (lax.rem(i, 2) == 0), of_three == 0)

        @pl.when(busy & starts & (q == 0))
        def _():
            tile_wait(t)

        pl.when((i == CHIPS + 2) & (n < ROUNDS - PER_TILE))(lambda: tile(t + CHIPS + 1))

        tick(n - AHEAD)

        @pl.when(makes(n - 1))
        def _():
            put(0, 0).wait()
            put(1, 0).wait()

        pl.when((i == 1) & (n >= PER_TILE) & (n < ROUNDS + PER_TILE))(lambda: put_d(0, lambda d: d.wait()))
        begin_round(n - AHEAD)

        ends = busy & ~early & (of_three == 2)
        inner, turning = t < CHIPS, (t == CHIPS) & (i < CHIPS)
        before = q < 2
        share = (jnp.where(before, 1 - slot, slot), part(lax.rem(q, 2), half), before.astype(jnp.int32))
        own_share = (slot, part(lax.div(i - 2 * CHIPS, 2), half), 0)
        late = (t == 0) & (i >= 2 * CHIPS)

        @pl.when(turning)
        def _():
            for which in range(2):
                by_normed(which, 1 - slot, part(i, PIECE), 1)
            next_layer(i)

        pl.when(busy & starts)(lambda: tokens(slot, q))

        @pl.when(makes(n) & early)
        def _():
            wide_terms(dgate, 0, q)
            wide_terms(dup, 1, q)
            down_terms(q)
            puts(t, q)

        for which in range(2):
            pl.when(late & (lax.rem(i, 2) == which))(lambda which=which: by_normed(which, *own_share))

        @pl.when(makes(n) & ~early & inner)
        def _():
            wide_terms(dgate, 0, q)
            wide_terms(dup, 1, q)
            by_normed(0, *share)
            puts(t, q)

        @pl.when(makes(n) & ~early & ~inner)
        def _():
            wide_terms(dgate, 0, q)
            wide_terms(dup, 1, q)
            puts(t, q)

        @pl.when(ends & inner)
        def _():
            down_terms(q)
            by_normed(1, *share)

        pl.when(ends & ~inner)(lambda: down_terms(q))
        pl.when(busy & (i == PER_TILE - 1))(lambda: put_d(t, lambda d: d.start()))
        pl.when((n >= ROUNDS) & (n < ROUNDS + 2 * DEVICES))(lambda: keep(n - ROUNDS))

    states_kept(lambda d: d.wait())
    for number, rounds in enumerate((PER_TILE, PER_TILE, DEVICES, DEVICES, DEVICES)):
        some = pl.ds(0, rounds)
        pltpu.make_async_copy(news.at[some], terms.at[some], sem_keep.at[number]).wait()


def in_hbm(arrays):
    return [pltpu.with_memory_space_constraint(a, pltpu.HBM) for a in arrays]


def backward(x, dy, weights, m, v):
    def dma(*shape):
        return pltpu.SemaphoreType.DMA(shape)

    def bf(*shape):
        return pltpu.VMEM(shape, BF)

    def f32(*shape):
        return pltpu.VMEM(shape, F32)

    message = (MR, LANE)
    outs = ((2, CHIPS, *message), message, (2, CHIPS, *message))
    anywhere = pl.BlockSpec(memory_space=pltpu.HBM)
    return pl.pallas_call(
        kernel,
        name="backward",
        out_shape=[*[jax.ShapeDtypeStruct((ROUNDS, *s), BF) for s in outs], bf(T, TILE), bf(T, TILE), bf(T, TILE), f32(T, D), bf(D, T), bf(D, T)],
        in_specs=[anywhere] * 11,
        out_specs=[anywhere] * len(outs) + [pl.BlockSpec(memory_space=pltpu.VMEM)] * 6,
        scratch_shapes=[
            bf(KEPT, CHIPS, *message), bf(KEPT, CHIPS, *message), bf(CHIPS + 1, RING, *message), bf(3, SLOTS, *message), bf(SLOTS, *message), bf(SLOTS, *message),
            bf(*message), f32(*message), f32(*message), bf(SUB, D), f32(SUB, D), f32(SUB, D),
            bf(T, D), bf(T, D), bf(T, D), bf(T, D),
            bf(2, D, TILE), bf(2, D, TILE), bf(2, TILE, D),
            f32(T, D),
            bf(2, 2, CHIPS, *message), bf(CHIPS, 2, CHIPS, *message),
            dma(SLOTS), dma(KEPT), dma(3, SLOTS), dma(CHIPS + 1, RING), dma(KEPT), dma(3, 2), dma(5, SLOTS),
            dma(3, SLOTS), dma(CHIPS, RING), dma(3, SLOTS), dma(CHIPS, RING), dma(RING),
            dma(3), dma(3, 2), dma(2 + CHIPS), dma(9),
        ],
        compiler_params=pltpu.CompilerParams(collective_id=0, has_side_effects=True, vmem_limit_bytes=67_043_328 - KEEP),
    )(*in_hbm((x, dy, *weights, *m, *v)))


DEPTH, STORES = 3, 2


def finish_kernel(*refs):
    def three(first):
        return refs[first : first + 3]

    news, grads, m, v = refs[0], refs[1], three(2), three(5)
    act, dgate, dup, dag, at, ctt = refs[8:14]
    w_out, m_out, v_out = three(14), three(17), three(20)
    new_in, grad_in, m_in, v_in = three(23), three(26), refs[29:31], refs[31:33]
    w_to, m_to, v_to = three(33), three(36), three(39)
    sem_in, sem_out = refs[42:]
    steps = 2 * DEVICES

    def where(i):
        n, d = 1 - lax.rem(i, 2), lax.div(i, 2)
        wide, tall = pl.ds(pl.multiple_of(PIECE * d, PIECE), PIECE), pl.ds(pl.multiple_of(2 * SUB * d, 2 * SUB), 2 * SUB)
        return n, d, [(n, slice(None), wide)] * 2 + [(n, tall)]

    def loads(i, go):
        slot = lax.rem(i, DEPTH)
        n, d, states = where(i)
        core, chip, of = lax.rem(d, 2), lax.div(d, 2), 1 - n
        for kind in range(3):
            if kind < 2:
                pairs = [(grads.at[of, :, kind, chip], grad_in[kind]), (m[kind].at[states[kind]], m_in[kind]), (v[kind].at[states[kind]], v_in[kind])]
            else:
                pairs = [(grads.at[of, chip, kind, pl.ds(2 * core, 2)], grad_in[kind])]
            for number, (src, dst) in enumerate(pairs):
                go(pltpu.make_async_copy(src, dst.at[slot], sem_in.at[slot, kind, number]))

        @pl.when(n == 0)
        def _():
            for kind in range(3):
                go(pltpu.make_async_copy(news.at[of, :, kind, :, core, chip], new_in[kind].at[slot], sem_in.at[slot, kind, 3]))

    def stores(i, go):
        slot = lax.rem(i, STORES)
        n, d, states = where(i)
        rows, tall = pl.ds(pl.multiple_of(ROWS * d, 16), ROWS), pl.ds(pl.multiple_of(TALL * d, TALL), TALL)
        for kind in range(3):
            pairs = (
                (w_to[kind], w_out[kind].at[n, rows if kind < 2 else tall]),
                (m_to[kind], m_out[kind].at[states[kind]]),
                (v_to[kind], v_out[kind].at[states[kind]]),
            )
            for number, (src, dst) in enumerate(pairs):
                go(pltpu.make_async_copy(src.at[slot], dst, sem_out.at[slot, kind, number]))

    for first in range(DEPTH):
        loads(first, lambda d: d.start())

    @times(steps)
    def _(i):
        slot, to = lax.rem(i, DEPTH), lax.rem(i, STORES)
        n, d, _ = where(i)
        loads(i, lambda c: c.wait())
        pl.when(i >= STORES)(lambda: stores(i - STORES, lambda c: c.wait()))

        def wide(kind, message):
            for j in range(CHIPS):
                for q in range(CHIPS):
                    for half in range(2):
                        w_to[kind][to, :, cut(4 * (2 * q + half) + j, LANE)] = message(j, q, half)

        def tall(message):
            for number in range(D // LANE):
                for j in range(CHIPS):
                    for q in range(CHIPS):
                        w_to[2][to, cut(CHIPS * j + q, SUB), cut(number, LANE)] = message(j, q, number)

        @pl.when(n == 0)
        def _():
            for kind in range(2):
                wide(kind, lambda j, q, half, kind=kind: new_in[kind][slot, j, q, cut(half, ROWS)])
            tall(lambda j, q, number: new_in[2][slot, j, q, cut(number, SUB)])

        for place, buf in enumerate((act, dgate, dup)):

            @pl.when((n == 1) & (lax.div(d, 3) == place))
            def _(buf=buf):
                for kind in range(2):

                    def message(j, q, half, kind=kind):
                        row = MR * (CHIPS * lax.rem(d, 3) + 2 * kind + j // 2) + ROWS * half
                        return buf[pl.ds(pl.multiple_of(row, 16), ROWS), cut(CHIPS * (j % 2) + q, LANE)]

                    wide(kind, message)

        for place, buf in enumerate((at, ctt)):

            @pl.when((n == 1) & (lax.div(d, CHIPS) == place))
            def _(buf=buf):
                def message(j, q, number):
                    return buf[pl.ds(pl.multiple_of(MR * lax.rem(d, CHIPS) + SUB * number, SUB), SUB), cut(CHIPS * j + q, LANE)]

                tall(message)

        s = lax.rem(d, 2)
        for kind in range(2):
            for j in range(CHIPS):
                cols = cut(j, LANE)
                old_m, old_v = m_in[kind][slot, :, cols], v_in[kind][slot, :, cols]
                g = grad_in[kind][slot, j, part(s, ROWS)].astype(F32)
                m_to[kind][to, :, cols], v_to[kind][to, :, cols] = moments(old_m, old_v, g)
        for number in range(D // LANE):
            for q in range(2):
                cols, row = cut(number, LANE), TALL * n + 2 * SUB * d + SUB * q
                old_m = dag[pl.ds(pl.multiple_of(row, SUB), SUB), cols]
                old_v = dag[pl.ds(pl.multiple_of(row + 2 * TALL, SUB), SUB), cols]
                g = grad_in[2][slot, q, cut(number, SUB)].astype(F32)
                m_to[2][to, cut(q, SUB), cols], v_to[2][to, cut(q, SUB), cols] = moments(old_m, old_v, g)
        stores(i, lambda c: c.start())
        pl.when(i < steps - DEPTH)(lambda: loads(i + DEPTH, lambda c: c.start()))

    for last in range(STORES):
        stores(steps - STORES + last, lambda c: c.wait())


def finish(news, grads, m, v, kept):
    shape = (2, CHIPS, 3, CHIPS)
    news, grads = news.reshape(*shape, 2, CHIPS, MR, LANE), grads.reshape(*shape, MR, LANE)
    anywhere, here = pl.BlockSpec(memory_space=pltpu.HBM), pl.BlockSpec(memory_space=pltpu.VMEM)
    blocks = [(ROWS, PIECE), (ROWS, PIECE), (2 * SUB, D)]
    states = [jax.ShapeDtypeStruct(a.shape, F32) for a in m]
    return pl.pallas_call(
        finish_kernel,
        name="finish",
        out_shape=[*[jax.ShapeDtypeStruct((2, D, FF), BF)] * 2, jax.ShapeDtypeStruct((2, FF, D), BF), *states * 2],
        in_specs=[anywhere] * 8 + [here] * len(kept),
        out_specs=[anywhere] * 9,
        scratch_shapes=[
            *[pltpu.VMEM((DEPTH, CHIPS, CHIPS, MR, LANE), BF)] * 3,
            *[pltpu.VMEM((DEPTH, n, MR, LANE), BF) for n in (CHIPS, CHIPS, 2)],
            *[pltpu.VMEM((DEPTH, *blocks[0]), F32)] * 4,
            *[pltpu.VMEM((STORES, *b), BF) for b in ((ROWS, FF), (ROWS, FF), (TALL, D))],
            *[pltpu.VMEM((STORES, *b), F32) for b in blocks * 2],
            pltpu.SemaphoreType.DMA((DEPTH, 3, 4)), pltpu.SemaphoreType.DMA((STORES, 3, 3)),
        ],
        compiler_params=pltpu.CompilerParams(vmem_limit_bytes=18 * 2**20),
    )(*in_hbm((news, grads, *m, *v)), *[pltpu.with_memory_space_constraint(a, pltpu.VMEM) for a in kept])


def solution(mesh):
    def step(x, dy, *arrays):
        weights, m, v = (arrays[i : i + 3] for i in (0, 3, 6))
        news, grads, _, *kept = backward(x[0], dy[0], weights, m, v)
        return tuple(finish(news, grads, m, v, kept))

    by_device, whole, rows = P(("rep", "dp")), P(), P(None, "dp")
    return jax.shard_map(
        step,
        mesh=mesh,
        in_specs=(by_device,) * 2 + (whole,) * 3 + (rows,) * 6,
        out_specs=(P("rep"),) * 3 + (P("rep", "dp"),) * 6,
        check_vma=False,
    )
```

```python
import jax
import jax.numpy as jnp
from jax import lax
from jax.experimental import pallas as pl
from jax.experimental.pallas import tpu as pltpu
from jax.sharding import PartitionSpec as P

MESH = pl.DeviceIdType.MESH
BF, F32 = jnp.bfloat16, jnp.float32

T, D, FF = 2048, 640, 4096
DEVICES, CHIPS, LANE = 8, 4, 128
TILE = DEVICES * LANE
ROWS, TALL = D // DEVICES, FF // DEVICES
PIECE, BLOCK = 512, 256
PARTS = 2
KEEP = 2 * 3 * T * TILE + 2 * 2 * D * T + 4 * T * D

ROUNDS, MR, SUB = 96, 160, 32
PER_TILE = 12
D0, LAG, LAGF, LAGA, LAGD = 1, 2, 3, 3, 2
RING, SLOTS, KEPT = 16, 4, 12
TICKS = ROUNDS + D0 + 3 * LAG + LAGF + 2 * LAGA + max(LAGD, SLOTS)
AHEAD = 6


def normed(h):
    wide = h.astype(F32)
    scale = lax.rsqrt(jnp.mean(wide**2, -1, keepdims=True) + 1e-6)
    return (wide * scale).astype(BF)


def dot(a, b):
    return jnp.dot(a, b, preferred_element_type=F32)


def across(a, b):
    return lax.dot_general(a, b, (((1,), (1,)), ((), ())), preferred_element_type=F32)


def moments(m, v, g):
    return 0.9 * m + 0.1 * g, 0.95 * v + 0.05 * g * g


def within(r):
    return (r >= 0) & (r < ROUNDS)


def stage(n):
    t = lax.div(n, PER_TILE)
    return t, lax.rem(n, PER_TILE), lax.rem(t, CHIPS) == 0


def plan(r):
    t, i, early = stage(r + CHIPS)
    late = i - CHIPS
    kind = jnp.where(early, jnp.where(late < 0, 2, lax.rem(late, 2)), lax.rem(i, 3))
    q = jnp.where(early, jnp.where(late < 0, i, lax.div(late, 2)), lax.div(i, 3))
    t = t - lax.div(kind, 2)
    return PER_TILE * t + CHIPS * kind + q, t, kind, q


def ends_kind(r):
    _, i, early = stage(r + CHIPS)
    return jnp.where(early, (i == 3) | (i >= PER_TILE - 2), i >= PER_TILE - 3)


def most(zp):
    return jnp.maximum(zp, CHIPS - 1 - zp)


def part(i, n):
    return pl.ds(pl.multiple_of(n * i, n), n)


def cut(i, n):
    return slice(n * i, n * i + n)


def times(n, first=0):
    return pl.loop(first, n)


def kernel(
    x, dy, w_g, w_u, w_d, m_g, m_u, m_d, v_g, v_u, v_d,
    news, grads, terms, act, dgate, dup, dag, at, ctt,
    mine, others, line, summed, fresh, final, wb, mb, vb, wdb, mdb, vdb,
    hv, xv, av, ct, wgt, wut, wdt, dau, staged, staged_d,
    sem_pair_s, sem_pair_r, sem_line_s, sem_line_r, sem_mine, sem_state, sem_own, sem_ag_s, sem_ag_r, sem_agp_s, sem_agp_r, sem_own_r,
    sem_in, sem_w, sem_st, sem_keep,
):
    def tile(t):
        slot, of, j = lax.rem(t, 2), lax.rem(lax.div(t, CHIPS), 2), lax.rem(t, CHIPS)
        sems = [sem_w.at[i, slot] for i in range(3)]
        for d in range(DEVICES):
            cols, to = pl.ds(pl.multiple_of(TALL * d + LANE * j, LANE), LANE), pl.ds(LANE * d, LANE)
            pltpu.make_async_copy(w_g.at[of, :, cols], wgt.at[slot, :, to], sems[0]).start()
            pltpu.make_async_copy(w_u.at[of, :, cols], wut.at[slot, :, to], sems[1]).start()
            pltpu.make_async_copy(w_d.at[of, cols], wdt.at[slot, to], sems[2]).start()

    def plain_tile(t):
        slot, cols = lax.rem(t, 2), part(t, TILE)
        for i, (src, dst) in enumerate(((w_g.at[0, :, cols], wgt), (w_u.at[0, :, cols], wut), (w_d.at[0, cols], wdt))):
            pltpu.make_async_copy(src, dst.at[slot], sem_w.at[i, slot]).start()

    def tile_wait(t):
        slot, all_of = lax.rem(t, 2), pl.ds(0, TILE)
        sems = [sem_w.at[i, slot] for i in range(3)]
        pltpu.make_async_copy(w_g.at[0, :, all_of], wgt.at[slot], sems[0]).wait()
        pltpu.make_async_copy(w_u.at[0, :, all_of], wut.at[slot], sems[1]).wait()
        pltpu.make_async_copy(w_d.at[0, all_of], wdt.at[slot], sems[2]).wait()

    upper, lower = pl.ds(0, T // 2), pl.ds(T // 2, T // 2)
    load_x, load_more = (pltpu.make_async_copy(x.at[rows], xv.at[rows], sem_in.at[i]) for i, rows in enumerate((upper, lower)))
    load_dy = pltpu.make_async_copy(dy, ct, sem_in.at[2])
    load_x.start()
    plain_tile(0)
    load_more.start()
    load_dy.start()
    plain_tile(1)

    line[...] = jnp.zeros_like(line)
    me = lax.axis_index("dp")
    z, c = lax.div(me, 2), lax.rem(me, 2)
    partner = me + 1 - 2 * c
    low, high = z > 0, z < CHIPS - 1

    barrier = pltpu.get_barrier_semaphore()

    def greet(dev):
        pl.semaphore_signal(barrier, inc=1, device_id={"dp": dev}, device_id_type=MESH)

    greet(partner)
    pl.when(low)(lambda: greet(me - 2))
    pl.when(high)(lambda: greet(me + 2))

    def remote(src, dst, send, recv, dev):
        return pltpu.make_async_remote_copy(src, dst, send, recv, device_id={"dp": dev}, device_id_type=MESH)

    def pair(r, at_round=0):
        slot, kept = lax.rem(r, SLOTS), lax.rem(r, KEPT)
        return remote(terms.at[at_round, 1 - c], others.at[kept], sem_pair_s.at[slot], sem_pair_r.at[kept], partner)

    def own_terms(r, at_round=0):
        kept = lax.rem(r, KEPT)
        return pltpu.make_async_copy(terms.at[at_round, c], mine.at[kept], sem_mine.at[kept])

    def arrival(r, place):
        ring = lax.rem(r, RING)
        return remote(summed.at[0, 0], line.at[place, ring], sem_line_s.at[0, 0], sem_line_r.at[place, ring], partner)

    def on_chip(r, zp):
        kept = lax.rem(r, KEPT)
        return mine[kept, zp].astype(F32) + others[kept, zp].astype(F32)

    class Line:
        def __init__(self, i, k):
            self.i, self.zp = i, lax.rem(z + 1 + i, CHIPS)
            self.right = self.zp > z
            self.r = k - D0 - LAG * jnp.where(self.right, z, CHIPS - 1 - z)
            self.ok = within(self.r)
            self.fed = self.ok & jnp.where(self.right, low, high)

        def send(self, r):
            nxt = jnp.where(self.right, z + 1, z - 1)
            place = jnp.where((nxt == self.zp) & ~self.right, CHIPS, self.zp)
            slot, ring = lax.rem(r, SLOTS), lax.rem(r, RING)
            return remote(summed.at[self.i, slot], line.at[place, ring], sem_line_s.at[self.i, slot], sem_line_r.at[place, ring], 2 * nxt + c)

        def step(self):
            pl.when(within(self.r - SLOTS))(lambda: self.send(self.r - SLOTS).wait_send())
            pl.when(self.fed)(lambda: arrival(self.r, self.zp).wait_recv())

            @pl.when(self.ok)
            def _():
                total = on_chip(self.r, self.zp) + line[self.zp, lax.rem(self.r, RING)].astype(F32)
                summed[self.i, lax.rem(self.r, SLOTS)] = total.astype(BF)
                self.send(self.r).start()

    def state(r, go):
        _, t, kind, q = plan(r)
        of, j = 1 - lax.div(t, CHIPS), lax.rem(t, CHIPS)
        for number, (w, m, v) in enumerate(((w_g, m_g, v_g), (w_u, m_u, v_u))):

            @pl.when(kind == number)
            def _(w=w, m=m, v=v):
                rows = pl.ds(pl.multiple_of(ROWS * me, 16), ROWS)
                for s in range(2):
                    cols = pl.ds(pl.multiple_of(TALL * (2 * q + s) + LANE * j, LANE), LANE)
                    to, sems = pl.ds(ROWS * s, ROWS), [sem_state.at[i, s] for i in range(3)]
                    go(pltpu.make_async_copy(w.at[of, rows, cols], wb.at[to], sems[0]))
                    go(pltpu.make_async_copy(m.at[of, :, cols], mb.at[to], sems[1]))
                    go(pltpu.make_async_copy(v.at[of, :, cols], vb.at[to], sems[2]))

        @pl.when(kind == 2)
        def _():
            row, sems = pl.multiple_of(LANE * j + SUB * q, SUB), [sem_state.at[i, 0] for i in range(3)]
            rows = pl.ds(row, SUB)
            go(pltpu.make_async_copy(w_d.at[of, pl.ds(pl.multiple_of(TALL * me + row, SUB), SUB)], wdb, sems[0]))
            go(pltpu.make_async_copy(m_d.at[of, rows], mdb, sems[1]))
            go(pltpu.make_async_copy(v_d.at[of, rows], vdb, sems[2]))

    def adamw(w, m, v, g):
        m, v = moments(m, v, g.astype(F32))
        w = w.astype(F32)
        return (w - 0.02 * (m * lax.rsqrt(v + 1e-8) + 0.1 * w)).astype(BF)

    class Own:
        def __init__(self, k):
            self.r = k - D0 - LAG * most(z)
            self.ok = within(self.r)

        def outs(self, r, go, at_round=0):
            slot, ring = lax.rem(r, SLOTS), lax.rem(r, RING)
            src, dst = fresh.at[slot], news.at[at_round, c, z]
            pl.when(high)(lambda: go(remote(src, dst, sem_own.at[0, slot], sem_ag_r.at[z, ring], me + 2)))
            pl.when(low)(lambda: go(remote(src, dst, sem_own.at[1, slot], sem_ag_r.at[z, ring], me - 2)))
            go(remote(src, dst, sem_own.at[2, slot], sem_own_r.at[ring], partner))

        def local(self, r, go, at_round=0):
            slot = lax.rem(r, SLOTS)
            go(pltpu.make_async_copy(fresh.at[slot], news.at[at_round, c, z], sem_own.at[3, slot]))
            go(pltpu.make_async_copy(final.at[slot], grads.at[at_round], sem_own.at[4, slot]))

        def step(self):
            @pl.when(within(self.r - SLOTS))
            def _():
                self.outs(self.r - SLOTS, lambda d: d.wait_send())
                self.local(self.r - SLOTS, lambda d: d.wait())

            pl.when(self.ok & low)(lambda: arrival(self.r, z).wait_recv())
            pl.when(self.ok & high)(lambda: arrival(self.r, CHIPS).wait_recv())

            @pl.when(self.ok)
            def _():
                slot, ring = lax.rem(self.r, SLOTS), lax.rem(self.r, RING)
                at_round, _, kind, _ = plan(self.r)
                total = on_chip(self.r, z) + line[z, ring].astype(F32) + line[CHIPS, ring].astype(F32)
                final[slot] = total.astype(BF)
                state(self.r, lambda d: d.wait())

                @pl.when(kind == 2)
                def _():
                    for i in range(D // LANE):
                        rows, cols = pl.ds(SUB * i, SUB), pl.ds(LANE * i, LANE)
                        fresh[slot, rows] = adamw(wdb[:, cols], mdb[:, cols], vdb[:, cols], final[slot, rows])

                @pl.when(kind < 2)
                def _():
                    fresh[slot] = adamw(wb[...], mb[...], vb[...], final[slot])

                self.outs(self.r, lambda d: d.start(), at_round)
                self.local(self.r, lambda d: d.start(), at_round)

            pl.when(within(self.r + 1))(lambda: state(self.r + 1, lambda d: d.start()))

    def sent(k, zp):
        away = jnp.abs(z - zp)
        return k - D0 - LAG * most(zp) - LAGA * away - (LAGF - LAGA) * jnp.minimum(away, 1)

    class Gather:
        def __init__(self, i, k):
            self.i, self.zp = i, lax.rem(z + 1 + i, CHIPS)
            self.r, self.up = sent(k, self.zp), self.zp < z
            self.on = jnp.where(self.up, high, low)

        def forward(self, r, at_round=0):
            nxt, spot = jnp.where(self.up, z + 1, z - 1), news.at[at_round, c, self.zp]
            return remote(spot, spot, sem_ag_s.at[self.i, lax.rem(r, SLOTS)], sem_ag_r.at[self.zp, lax.rem(r, RING)], 2 * nxt + c)

        def over(self, r, at_round=CHIPS - 1):
            return bundle(r, at_round, c, self.zp, sem_agp_s.at[self.i, lax.rem(r, SLOTS)])

        def step(self):
            r, old, now = self.r, within(self.r - SLOTS), within(self.r)
            pl.when(old & self.on)(lambda: self.forward(r - SLOTS).wait_send())
            pl.when(old & ends_kind(r - SLOTS))(lambda: self.over(r - SLOTS).wait_send())

            @pl.when(now)
            def _():
                self.forward(r).wait_recv()
                at_round, _, _, q = plan(r)
                pl.when(self.on)(lambda: self.forward(r, at_round).start())
                pl.when(q == CHIPS - 1)(lambda: self.over(r, at_round).start())

    def bundle(r, at_round, core, zp, send):
        spot = news.at[pl.ds(at_round - (CHIPS - 1), CHIPS), core, zp]
        return remote(spot, spot, send, sem_agp_r.at[zp, lax.rem(r, RING)], partner)

    def tick(k):
        pl.when(within(k - SLOTS))(lambda: pair(k - SLOTS).wait_send())

        @pl.when(within(k - D0))
        def _():
            pair(k - D0).wait_recv()
            own_terms(k - D0).wait()

        for i in range(CHIPS - 1):
            Gather(i, k).step()
        for i in range(CHIPS - 1):
            Line(i, k).step()
        Own(k).step()
        r = sent(k, z) - LAGD
        spot = news.at[0, 1 - c, z]
        pl.when(within(r))(lambda: remote(spot, spot, sem_agp_s.at[0, 0], sem_own_r.at[lax.rem(r, RING)], partner).wait_recv())
        for i in range(CHIPS - 1):
            zp = lax.rem(z + 1 + i, CHIPS)
            r = sent(k, zp) - LAGD
            done = within(r) & ends_kind(r)
            pl.when(done)(lambda r=r, zp=zp: bundle(r, CHIPS - 1, 1 - c, zp, sem_agp_s.at[0, 0]).wait_recv())

    def begin_round(k):
        @pl.when(within(k))
        def _():
            at_round = plan(k)[0]
            pair(k, at_round).start()
            own_terms(k, at_round).start()

    half = T // 2
    blocks = half // BLOCK

    def enter(p):
        rows = part(p, BLOCK)
        av[rows] = normed(xv[rows])
        dag[rows] = jnp.zeros((BLOCK, D), F32)

    def hidden(t, p):
        slot, rows = lax.rem(t, 2), pl.ds(half * p, half)
        a = av[rows]
        for n in range(TILE // PIECE):
            cols = pl.ds(PIECE * n, PIECE)
            gate, up = dot(a, wgt[slot, :, cols]), dot(a, wut[slot, :, cols])
            act[rows, cols] = (gate * jax.nn.sigmoid(gate) * up).astype(BF)

    def turn(i):
        rows = part(i, BLOCK)
        ctt[:, rows] = ct[rows].T

    def back(t, p, n=half):
        rows = pl.ds(n * p, n)
        dag[rows] = dag[rows] + dot(act[rows], wdt[lax.rem(t, 2)])

    def leave(p):
        rows = part(p, BLOCK)
        h = xv[rows] + dag[rows].astype(BF)
        a = normed(h)
        hv[rows], av[rows], at[:, rows] = h, a, a.T
        dag[rows] = dau[rows] = jnp.zeros((BLOCK, D), F32)

    load_x.wait()
    times(blocks)(enter)
    tile_wait(0)
    load_more.wait()
    hidden(0, 0)
    for p in range(blocks):
        enter(blocks + p)
    load_dy.wait()
    turn(0)
    back(0, 0)
    hidden(0, 1)
    turn(1)

    @times(CHIPS, first=1)
    def _(t):
        tile_wait(t)
        back(t - 1, 1)
        hidden(t, 0)
        turn(2 * t)
        pl.when(t < CHIPS - 1)(lambda: plain_tile(t + 1))
        pl.when(t == CHIPS - 1)(lambda: tile(t + 1))
        back(t, 0)
        hidden(t, 1)
        turn(2 * t + 1)

    for third in range(2):
        back(CHIPS - 1, 2 + third, PIECE)
        for p in range(3):
            leave(3 * third + p)
    times(2 * blocks, first=2 * blocks - 2)(leave)

    def next_layer(q):
        @times(PIECE // BLOCK)
        def _(i):
            rows = part(PIECE // BLOCK * q + i, BLOCK)
            da = (dag[rows].astype(BF) + dau[rows].astype(BF)).astype(F32)
            wide = hv[rows].astype(F32)
            mean = jnp.mean(wide * wide, -1, keepdims=True) + 1e-6
            scale = lax.rsqrt(mean)
            along = jnp.sum(da * wide, -1, keepdims=True) * (-scale / (D * mean))
            by = ct[rows] + (da * scale + wide * along).astype(BF)
            a = normed(xv[rows])
            ct[rows], ctt[:, rows], av[rows], at[:, rows] = by, by.T, a, a.T

    def tokens(slot, q):
        cols = part(q, BLOCK)
        for p in range(PARTS):
            rows = pl.ds(T // PARTS * p, T // PARTS)
            a, by = av[rows], ct[rows]
            gate, up = dot(a, wgt[slot, :, cols]), dot(a, wut[slot, :, cols])
            dact = across(by, wdt[slot, cols]).astype(BF).astype(F32)
            sig = jax.nn.sigmoid(gate)
            silu = gate * sig
            act[rows, cols] = (silu * up).astype(BF)
            dup[rows, cols] = (dact * silu).astype(BF)
            dgate[rows, cols] = (dact * up * (sig + silu * (1.0 - sig))).astype(BF)

    def put(kind, r):
        return pltpu.make_async_copy(staged.at[kind], terms.at[r], sem_st.at[kind])

    def put_d(t, go):
        for q in range(CHIPS):
            go(pltpu.make_async_copy(staged_d.at[q], terms.at[PER_TILE * t + 2 * CHIPS + q], sem_st.at[2 + q]))

    def wide_terms(by, kind, q):
        g = dot(at[...], by[:, part(q, BLOCK)]).astype(BF)
        for d in range(DEVICES):
            for s in range(2):
                staged[kind, d % 2, d // 2, cut(s, ROWS)] = g[cut(d, ROWS), cut(s, LANE)]

    def puts(t, q):
        for kind in range(2):
            put(kind, PER_TILE * t + CHIPS * kind + q).start()

    def down_terms(i):
        g = dot(ctt[...], act[:, part(i, BLOCK)]).T.astype(BF)
        for o in range(2):
            for q in range(CHIPS):
                for s in range(D // LANE):
                    staged_d[q, o, i, cut(s, SUB)] = g[cut(CHIPS * o + q, SUB), cut(s, LANE)]

    sides = ((dag, dgate, wgt), (dau, dup, wut))

    def by_normed(which, slot, rows, side):
        (to, by, w), cols = sides[which], part(side, PIECE)
        to[rows] = to[rows] + across(by[rows, cols], w[slot, :, cols])

    pl.semaphore_wait(barrier, 1 + low.astype(jnp.int32) + high.astype(jnp.int32))

    def states_kept(go):
        for i, src in enumerate((m_d, v_d)):
            for of in range(2):
                place = 2 * i + of
                go(pltpu.make_async_copy(src.at[of], dag.at[cut(place, TALL)], sem_keep.at[5 + place]))

    def keep(e):
        d, kind = lax.div(e, 2), lax.rem(e, 2)
        core, chip = lax.rem(d, 2), lax.div(d, 2)
        pl.when(e == 0)(lambda: states_kept(lambda c: c.start()))

        def take(j, q, kind, buf, row, col, number):
            to = buf.at[pl.ds(pl.multiple_of(MR * row, MR), MR), cut(col, LANE)]
            pltpu.make_async_copy(news.at[PER_TILE * j + CHIPS * kind + q, core, chip], to, sem_keep.at[number]).start()

        for number, buf in enumerate((act, dgate, dup)):

            @pl.when(lax.div(d, 3) == number)
            def _(number=number, buf=buf):
                for j in range(CHIPS):
                    for q in range(CHIPS):
                        take(j, q, kind, buf, CHIPS * lax.rem(d, 3) + 2 * kind + j // 2, CHIPS * (j % 2) + q, number)

        for number, buf in enumerate((at, ctt)):

            @pl.when((kind == 0) & (lax.div(d, CHIPS) == number))
            def _(number=number, buf=buf):
                for j in range(CHIPS):
                    for q in range(CHIPS):
                        take(j, q, 2, buf, lax.rem(d, CHIPS), CHIPS * j + q, 3 + number)

    def makes(n):
        _, i, early = stage(n)
        return (n >= CHIPS) & (n < ROUNDS) & jnp.where(early, (i > CHIPS) & (lax.rem(i, 2) == 1), lax.rem(i, 3) == 1)

    @times(TICKS + AHEAD, first=CHIPS)
    def _(n):
        t, i, early = stage(n)
        slot, busy = lax.rem(t, 2), n < ROUNDS
        q = jnp.where(early, lax.div(jnp.maximum(i - CHIPS, 0), 2), lax.div(i, 3))
        of_three = lax.rem(i, 3)
        starts = jnp.where(early, (i >= CHIPS) & (lax.rem(i, 2) == 0), of_three == 0)

        @pl.when(busy & starts & (q == 0))
        def _():
            tile_wait(t)

        pl.when((i == CHIPS + 2) & (n < ROUNDS - PER_TILE))(lambda: tile(t + CHIPS + 1))

        tick(n - AHEAD)

        @pl.when(makes(n - 1))
        def _():
            put(0, 0).wait()
            put(1, 0).wait()

        pl.when((i == 1) & (n >= PER_TILE) & (n < ROUNDS + PER_TILE))(lambda: put_d(0, lambda d: d.wait()))
        begin_round(n - AHEAD)

        ends = busy & ~early & (of_three == 2)
        inner, turning = t < CHIPS, (t == CHIPS) & (i < CHIPS)
        before = q < 2
        share = (jnp.where(before, 1 - slot, slot), part(lax.rem(q, 2), half), before.astype(jnp.int32))
        own_share = (slot, part(lax.div(i - 2 * CHIPS, 2), half), 0)
        late = (t == 0) & (i >= 2 * CHIPS)

        @pl.when(turning)
        def _():
            for which in range(2):
                by_normed(which, 1 - slot, part(i, PIECE), 1)
            next_layer(i)

        pl.when(busy & starts)(lambda: tokens(slot, q))

        @pl.when(makes(n) & early)
        def _():
            wide_terms(dgate, 0, q)
            wide_terms(dup, 1, q)
            down_terms(q)
            puts(t, q)

        for which in range(2):
            pl.when(late & (lax.rem(i, 2) == which))(lambda which=which: by_normed(which, *own_share))

        @pl.when(makes(n) & ~early & inner)
        def _():
            wide_terms(dgate, 0, q)
            wide_terms(dup, 1, q)
            by_normed(0, *share)
            puts(t, q)

        @pl.when(makes(n) & ~early & ~inner)
        def _():
            wide_terms(dgate, 0, q)
            wide_terms(dup, 1, q)
            puts(t, q)

        @pl.when(ends & inner)
        def _():
            down_terms(q)
            by_normed(1, *share)

        pl.when(ends & ~inner)(lambda: down_terms(q))
        pl.when(busy & (i == PER_TILE - 1))(lambda: put_d(t, lambda d: d.start()))
        pl.when((n >= ROUNDS) & (n < ROUNDS + 2 * DEVICES))(lambda: keep(n - ROUNDS))

    states_kept(lambda d: d.wait())
    for number, rounds in enumerate((PER_TILE, PER_TILE, DEVICES, DEVICES, DEVICES)):
        some = pl.ds(0, rounds)
        pltpu.make_async_copy(news.at[some], terms.at[some], sem_keep.at[number]).wait()


def in_hbm(arrays):
    return [pltpu.with_memory_space_constraint(a, pltpu.HBM) for a in arrays]


def backward(x, dy, weights, m, v):
    def dma(*shape):
        return pltpu.SemaphoreType.DMA(shape)

    def bf(*shape):
        return pltpu.VMEM(shape, BF)

    def f32(*shape):
        return pltpu.VMEM(shape, F32)

    message = (MR, LANE)
    outs = ((2, CHIPS, *message), message, (2, CHIPS, *message))
    anywhere = pl.BlockSpec(memory_space=pltpu.HBM)
    return pl.pallas_call(
        kernel,
        name="backward",
        out_shape=[*[jax.ShapeDtypeStruct((ROUNDS, *s), BF) for s in outs], bf(T, TILE), bf(T, TILE), bf(T, TILE), f32(T, D), bf(D, T), bf(D, T)],
        in_specs=[anywhere] * 11,
        out_specs=[anywhere] * len(outs) + [pl.BlockSpec(memory_space=pltpu.VMEM)] * 6,
        scratch_shapes=[
            bf(KEPT, CHIPS, *message), bf(KEPT, CHIPS, *message), bf(CHIPS + 1, RING, *message), bf(3, SLOTS, *message), bf(SLOTS, *message), bf(SLOTS, *message),
            bf(*message), f32(*message), f32(*message), bf(SUB, D), f32(SUB, D), f32(SUB, D),
            bf(T, D), bf(T, D), bf(T, D), bf(T, D),
            bf(2, D, TILE), bf(2, D, TILE), bf(2, TILE, D),
            f32(T, D),
            bf(2, 2, CHIPS, *message), bf(CHIPS, 2, CHIPS, *message),
            dma(SLOTS), dma(KEPT), dma(3, SLOTS), dma(CHIPS + 1, RING), dma(KEPT), dma(3, 2), dma(5, SLOTS),
            dma(3, SLOTS), dma(CHIPS, RING), dma(3, SLOTS), dma(CHIPS, RING), dma(RING),
            dma(3), dma(3, 2), dma(2 + CHIPS), dma(9),
        ],
        compiler_params=pltpu.CompilerParams(collective_id=0, has_side_effects=True, vmem_limit_bytes=67_043_328 - KEEP),
    )(*in_hbm((x, dy, *weights, *m, *v)))


DEPTH, STORES = 3, 2


def finish_kernel(*refs):
    def three(first):
        return refs[first : first + 3]

    news, grads, m, v = refs[0], refs[1], three(2), three(5)
    act, dgate, dup, dag, at, ctt = refs[8:14]
    w_out, m_out, v_out = three(14), three(17), three(20)
    new_in, grad_in, m_in, v_in = three(23), three(26), refs[29:31], refs[31:33]
    w_to, m_to, v_to = three(33), three(36), three(39)
    sem_in, sem_out = refs[42:]
    steps = 2 * DEVICES

    def where(i):
        n, d = 1 - lax.rem(i, 2), lax.div(i, 2)
        wide, tall = pl.ds(pl.multiple_of(PIECE * d, PIECE), PIECE), pl.ds(pl.multiple_of(2 * SUB * d, 2 * SUB), 2 * SUB)
        return n, d, [(n, slice(None), wide)] * 2 + [(n, tall)]

    def loads(i, go):
        slot = lax.rem(i, DEPTH)
        n, d, states = where(i)
        core, chip, of = lax.rem(d, 2), lax.div(d, 2), 1 - n
        for kind in range(3):
            if kind < 2:
                pairs = [(grads.at[of, :, kind, chip], grad_in[kind]), (m[kind].at[states[kind]], m_in[kind]), (v[kind].at[states[kind]], v_in[kind])]
            else:
                pairs = [(grads.at[of, chip, kind, pl.ds(2 * core, 2)], grad_in[kind])]
            for number, (src, dst) in enumerate(pairs):
                go(pltpu.make_async_copy(src, dst.at[slot], sem_in.at[slot, kind, number]))

        @pl.when(n == 0)
        def _():
            for kind in range(3):
                go(pltpu.make_async_copy(news.at[of, :, kind, :, core, chip], new_in[kind].at[slot], sem_in.at[slot, kind, 3]))

    def stores(i, go):
        slot = lax.rem(i, STORES)
        n, d, states = where(i)
        rows, tall = pl.ds(pl.multiple_of(ROWS * d, 16), ROWS), pl.ds(pl.multiple_of(TALL * d, TALL), TALL)
        for kind in range(3):
            pairs = (
                (w_to[kind], w_out[kind].at[n, rows if kind < 2 else tall]),
                (m_to[kind], m_out[kind].at[states[kind]]),
                (v_to[kind], v_out[kind].at[states[kind]]),
            )
            for number, (src, dst) in enumerate(pairs):
                go(pltpu.make_async_copy(src.at[slot], dst, sem_out.at[slot, kind, number]))

    for first in range(DEPTH):
        loads(first, lambda d: d.start())

    @times(steps)
    def _(i):
        slot, to = lax.rem(i, DEPTH), lax.rem(i, STORES)
        n, d, _ = where(i)
        loads(i, lambda c: c.wait())
        pl.when(i >= STORES)(lambda: stores(i - STORES, lambda c: c.wait()))

        def wide(kind, message):
            for j in range(CHIPS):
                for q in range(CHIPS):
                    for half in range(2):
                        w_to[kind][to, :, cut(4 * (2 * q + half) + j, LANE)] = message(j, q, half)

        def tall(message):
            for number in range(D // LANE):
                for j in range(CHIPS):
                    for q in range(CHIPS):
                        w_to[2][to, cut(CHIPS * j + q, SUB), cut(number, LANE)] = message(j, q, number)

        @pl.when(n == 0)
        def _():
            for kind in range(2):
                wide(kind, lambda j, q, half, kind=kind: new_in[kind][slot, j, q, cut(half, ROWS)])
            tall(lambda j, q, number: new_in[2][slot, j, q, cut(number, SUB)])

        for place, buf in enumerate((act, dgate, dup)):

            @pl.when((n == 1) & (lax.div(d, 3) == place))
            def _(buf=buf):
                for kind in range(2):

                    def message(j, q, half, kind=kind):
                        row = MR * (CHIPS * lax.rem(d, 3) + 2 * kind + j // 2) + ROWS * half
                        return buf[pl.ds(pl.multiple_of(row, 16), ROWS), cut(CHIPS * (j % 2) + q, LANE)]

                    wide(kind, message)

        for place, buf in enumerate((at, ctt)):

            @pl.when((n == 1) & (lax.div(d, CHIPS) == place))
            def _(buf=buf):
                def message(j, q, number):
                    return buf[pl.ds(pl.multiple_of(MR * lax.rem(d, CHIPS) + SUB * number, SUB), SUB), cut(CHIPS * j + q, LANE)]

                tall(message)

        s = lax.rem(d, 2)
        for kind in range(2):
            for j in range(CHIPS):
                cols = cut(j, LANE)
                old_m, old_v = m_in[kind][slot, :, cols], v_in[kind][slot, :, cols]
                g = grad_in[kind][slot, j, part(s, ROWS)].astype(F32)
                m_to[kind][to, :, cols], v_to[kind][to, :, cols] = moments(old_m, old_v, g)
        for number in range(D // LANE):
            for q in range(2):
                cols, row = cut(number, LANE), TALL * n + 2 * SUB * d + SUB * q
                old_m = dag[pl.ds(pl.multiple_of(row, SUB), SUB), cols]
                old_v = dag[pl.ds(pl.multiple_of(row + 2 * TALL, SUB), SUB), cols]
                g = grad_in[2][slot, q, cut(number, SUB)].astype(F32)
                m_to[2][to, cut(q, SUB), cols], v_to[2][to, cut(q, SUB), cols] = moments(old_m, old_v, g)
        stores(i, lambda c: c.start())
        pl.when(i < steps - DEPTH)(lambda: loads(i + DEPTH, lambda c: c.start()))

    for last in range(STORES):
        stores(steps - STORES + last, lambda c: c.wait())


def finish(news, grads, m, v, kept):
    shape = (2, CHIPS, 3, CHIPS)
    news, grads = news.reshape(*shape, 2, CHIPS, MR, LANE), grads.reshape(*shape, MR, LANE)
    anywhere, here = pl.BlockSpec(memory_space=pltpu.HBM), pl.BlockSpec(memory_space=pltpu.VMEM)
    blocks = [(ROWS, PIECE), (ROWS, PIECE), (2 * SUB, D)]
    states = [jax.ShapeDtypeStruct(a.shape, F32) for a in m]
    return pl.pallas_call(
        finish_kernel,
        name="finish",
        out_shape=[*[jax.ShapeDtypeStruct((2, D, FF), BF)] * 2, jax.ShapeDtypeStruct((2, FF, D), BF), *states * 2],
        in_specs=[anywhere] * 8 + [here] * len(kept),
        out_specs=[anywhere] * 9,
        scratch_shapes=[
            *[pltpu.VMEM((DEPTH, CHIPS, CHIPS, MR, LANE), BF)] * 3,
            *[pltpu.VMEM((DEPTH, n, MR, LANE), BF) for n in (CHIPS, CHIPS, 2)],
            *[pltpu.VMEM((DEPTH, *blocks[0]), F32)] * 4,
            *[pltpu.VMEM((STORES, *b), BF) for b in ((ROWS, FF), (ROWS, FF), (TALL, D))],
            *[pltpu.VMEM((STORES, *b), F32) for b in blocks * 2],
            pltpu.SemaphoreType.DMA((DEPTH, 3, 4)), pltpu.SemaphoreType.DMA((STORES, 3, 3)),
        ],
        compiler_params=pltpu.CompilerParams(vmem_limit_bytes=18 * 2**20),
    )(*in_hbm((news, grads, *m, *v)), *[pltpu.with_memory_space_constraint(a, pltpu.VMEM) for a in kept])


def solution(mesh):
    def step(x, dy, *arrays):
        weights, m, v = (arrays[i : i + 3] for i in (0, 3, 6))
        news, grads, _, *kept = backward(x[0], dy[0], weights, m, v)
        return tuple(finish(news, grads, m, v, kept))

    by_device, whole, rows = P(("rep", "dp")), P(), P(None, "dp")
    return jax.shard_map(
        step,
        mesh=mesh,
        in_specs=(by_device,) * 2 + (whole,) * 3 + (rows,) * 6,
        out_specs=(P("rep"),) * 3 + (P("rep", "dp"),) * 6,
        check_vma=False,
    )
```
